256 devices in a mesh: row: 16 (over x, y), col: 8 (over z), depth: 2 (over core).
Axes of the slice: x: 4, y: 4, z: 8, core: 2. Of those that a mesh axis runs over, the one named last changes fastest.
Arguments:
- halves: bfloat16 [2, 8192, 16384], P(None, 'row', ('col', 'depth')), may hold values from -6 to 6
- spectrum: float32 [2, 16384], P(None, ('col', 'depth')), as said below
- wanted: int32 [4096], P('col'), may hold values from 0 to 32766, as said below
- fraction: float32 [4096], P('col'), may hold values from 0.05 to 0.95
Outputs:
- eigvec: float32 [2, 8192, 4096], P(None, 'row', ('col', 'depth'))
The draws below stay inside these ranges and needn't reach their ends.
Inputs may be any that keep to these rules, and one draw needn't show every extreme that they name: Read in the order spectrum[0,0], spectrum[1,0], spectrum[0,1], spectrum[1,1], ... the values rise strictly, each by more than 0.05 over the one before. `wanted`: distinct positions in that merged order of the 32768 eigenvalues.
All inputs are finite; a program needn't handle non-finite values.
Results may differ from the reference program's by a relative error of at most 0.0029.
Values may be sent and summed in bfloat16 or wider, within the bound.
No kernel may reach another device: no remote copies, remote signals or barrier semaphores. Data moves between devices by JAX's collectives and lax.ppermute only.
A program may use at most 128 MiB of HBM per device.

```python
import math
import jax
import jax.numpy as jnp
from jax import lax

H = 16384
R = 8192
K = 4096


def draw_halves(key, part):
    noise_key = jax.random.fold_in(key, 11)
    random_part = jnp.clip(jax.random.normal(noise_key, (2, R, H), jnp.float32), -6.0, 6.0)
    values = random_part
    return values.astype(jnp.bfloat16)


def draw_spectrum(key, part):
    gaps = jnp.exp(jax.random.uniform(key, (2 * H,), jnp.float32, math.log(0.5), math.log(2.0)))
    ordered = jnp.cumsum(gaps)
    ordered = ordered - 0.5 * ordered[-1]
    return ordered.reshape(H, 2).T.astype(jnp.float32)


def draw_wanted(key, part):
    return jax.random.permutation(key, 2 * H - 1)[:K].astype(jnp.int32)


def level_of(key, extent, pieces, low, top_value):
    gain = 1.0
    for position, blocks in pieces:
        draws = jax.random.uniform(jax.random.fold_in(jax.random.fold_in(key, 6), position), (blocks,), jnp.float32, low / len(pieces), top_value / len(pieces))
        gain = gain * jnp.repeat(jnp.exp(draws), extent[position] // blocks).reshape((-1,) + (1,) * (len(extent) - 1 - position))
    return gain


def setup_inputs(seed: int = 0) -> dict:
    arg_keys = jax.random.split(jax.random.key(seed), 5)
    return {
        "halves": draw_halves(jax.random.fold_in(arg_keys[4], 71), 0),
        "spectrum": draw_spectrum(jax.random.fold_in(arg_keys[4], 71), 0),
        "wanted": draw_wanted(jax.random.fold_in(arg_keys[4], 71), 0),
        "fraction": jnp.clip(0.05 + 0.9 * jax.random.uniform(arg_keys[3], (K,), jnp.float32) ** level_of(arg_keys[3], (K,), ((0, 8),), -0.2, 0.2), 0.05, 0.95),
    }


def root_terms(spectrum, wanted):
    ordered = jnp.stack([spectrum[0], spectrum[1]], axis=1).reshape(-1)
    lower = jnp.take(ordered, wanted)
    upper = jnp.take(ordered, wanted + 1)
    return (lower, upper - lower)

def reference(halves, spectrum, wanted, fraction):
    seam = jnp.stack([halves[0, R - 1], halves[1, 0]]).astype(jnp.float32)
    lower, width = root_terms(spectrum, wanted)
    block = math.gcd(K, 512)
    count = K // block

    def one(index):
        start = (index * block).astype(jnp.int32)
        low = lax.dynamic_slice_in_dim(lower, start, block)
        wid = lax.dynamic_slice_in_dim(width, start, block)
        frc = lax.dynamic_slice_in_dim(fraction, start, block)
        cauchy = seam[:, :, None] / (spectrum[:, :, None] - low[None, None, :] - frc[None, None, :] * wid[None, None, :])
        norms = jnp.sqrt(lax.optimization_barrier(jnp.sum(cauchy * cauchy, axis=(0, 1))))
        rounded = cauchy.astype(jnp.bfloat16)
        first = jnp.dot(halves[0], rounded[0], preferred_element_type=jnp.float32)
        second = jnp.dot(halves[1], rounded[1], preferred_element_type=jnp.float32)
        return jnp.stack([first, second]) / norms[None, None, :]
    result = lax.map(one, jnp.arange(count).astype(jnp.int32))
    return jnp.transpose(result, (1, 2, 0, 3)).reshape(2, R, K)
```

```python
import functools

import jax
import jax.numpy as jnp
from jax import lax
from jax.experimental import pallas as pl
from jax.experimental.pallas import tpu as pltpu
from jax.sharding import Mesh
from jax.sharding import PartitionSpec as P

ROW = ("row_0", "row_1")
LANES = 128
PIECE = 64
F32 = jnp.float32
BF16 = jnp.bfloat16


def look_up(where_ref, blocks_ref, low_ref, shift_ref, *, steps, seam_row, root_row):
    core = where_ref[0]
    col = where_ref[1]
    count = blocks_ref.shape[0]
    rows = seam_row * 0 + root_row
    table = blocks_ref[:, :rows, :].reshape(count * rows, LANES)
    high = table.astype(BF16)
    rest = table - high.astype(F32)
    middle = rest.astype(BF16)
    small = (rest - middle.astype(F32)).astype(BF16)
    split = jnp.concatenate([high, middle, small], axis=1)
    per_block = rows * LANES
    half = per_block // 2
    row_ids = lax.broadcasted_iota(jnp.int32, (LANES, count * rows), 1)
    lane_ids = lax.broadcasted_iota(jnp.int32, (LANES, LANES), 1)

    def spot(position):
        owner = lax.shift_right_logical(position, per_block.bit_length() - 1)
        ahead = lax.shift_right_logical(owner, 1) - col
        ahead = jnp.where(core == 0, ahead, -ahead) & (count // 2 - 1)
        order = ahead * 2 + ((owner & 1) ^ core)
        inside = position & (per_block - 1)
        index = (inside & 1) * half + lax.shift_right_logical(inside, 1)
        return order * rows + lax.shift_right_logical(index, 7), index & (LANES - 1)

    for at, step in enumerate(steps):
        both = jnp.concatenate([blocks_ref[2 * step, root_row : root_row + 8, :], blocks_ref[2 * step + 1, root_row : root_row + 8, :]], axis=0)
        flipped = jnp.transpose(jnp.concatenate([both, jnp.zeros((LANES - 16, LANES), F32)], axis=0))
        for tile in range(2 if step == 0 else 4):
            base = (tile // 2) * 8 + tile % 2
            position = flipped[:, base : base + 1].astype(jnp.int32)
            fraction = flipped[:, base + 2 : base + 3]
            picks, masks = ([], [])
            for p in (position, position + 1):
                r, l = spot(p)
                picks.append(jnp.where(row_ids == r, 1.0, 0.0).astype(BF16))
                masks.append(lane_ids == l)
            got = jnp.dot(jnp.concatenate(picks, axis=0), split, preferred_element_type=F32)
            got = (got[:, :LANES] + got[:, LANES : 2 * LANES]) + got[:, 2 * LANES :]
            lower = jnp.sum(jnp.where(masks[0], got[:LANES], 0.0), axis=1, keepdims=True)
            upper = jnp.sum(jnp.where(masks[1], got[LANES:], 0.0), axis=1, keepdims=True)
            shift = fraction * (upper - lower)
            low_ref[at, tile * LANES : (tile + 1) * LANES, :] = jnp.broadcast_to(lower, (LANES, LANES))
            shift_ref[at, tile * LANES : (tile + 1) * LANES, :] = jnp.broadcast_to(shift, (LANES, LANES))


def roots_of(where, blocks, steps, root_row):
    n = len(steps)
    shape = jax.ShapeDtypeStruct((n, 4 * LANES, LANES), F32)
    return pl.pallas_call(
        functools.partial(look_up, steps=steps, seam_row=0, root_row=root_row),
        out_shape=(shape, shape),
        in_specs=[pl.BlockSpec(memory_space=pltpu.SMEM), pl.BlockSpec(memory_space=pltpu.VMEM)],
        out_specs=[pl.BlockSpec(memory_space=pltpu.VMEM)] * 2,
        cost_estimate=pl.CostEstimate(flops=n * 1024 * 256 * 384 * 2, bytes_accessed=4 << 20, transcendentals=0),
        name="look_up",
    )(where, blocks)


def multiply(which_ref, own_ref, other_ref, value_ref, seam_ref, low_ref, shift_ref, *refs, send):
    if send:
        out_ref, block_ref, square_ref = refs
    else:
        out_ref, norm_ref, block_ref, square_ref = refs
    columns = low_ref.shape[1]
    rows = own_ref.shape[1]
    width = own_ref.shape[2]
    tiles = width // LANES
    for part in range(columns // 256):
        for piece in range(256 // PIECE):
            start = part * 256 + piece * PIECE
            low = low_ref[0, start : start + PIECE, :]
            shift = shift_ref[0, start : start + PIECE, :]
            square = jnp.zeros((PIECE, LANES), F32)
            for source in range(2):
                for tile in range(tiles):
                    value = value_ref[source, 0, tile : tile + 1, :]
                    seam = seam_ref[source, 0, tile : tile + 1, :]
                    cauchy = seam / ((value - low) - shift)
                    square = square + cauchy * cauchy
                    block_ref[
                        start : start + PIECE, source * width + tile * LANES : source * width + (tile + 1) * LANES
                    ] = cauchy.astype(BF16)
            square_ref[start : start + PIECE, :] = square
        at = slice(part * 256, (part + 1) * 256)
        nt = (((1,), (1,)), ((), ()))
        product = lax.dot_general(own_ref[0], block_ref[at, :width], nt, preferred_element_type=F32)
        product = product + lax.dot_general(other_ref[0], block_ref[at, width:], nt, preferred_element_type=F32)
        norm = jnp.sum(jnp.transpose(square_ref[at, :]), axis=0, keepdims=True)
        if send:
            out_ref[:rows, at] = product.astype(BF16)
            put_norm(out_ref, rows, at, norm)
        else:
            out_ref[0, :, at] = product
            norm_ref[0, :, at] = jnp.broadcast_to(norm, (8, 256))


def put_norm(out_ref, rows, at, norm):
    high = norm.astype(BF16).astype(F32)
    row = lax.broadcasted_iota(jnp.int32, (16, norm.shape[1]), 0)
    both = jnp.where(row == 0, high, jnp.where(row == 1, norm - high, 0.0))
    out_ref[rows : rows + 16, at] = both.astype(BF16)


def products(which, own, other, value, seam, low, shift, at, columns, send):
    n = which.shape[0]
    rows, width = own.shape[1:]
    tiles = width // LANES
    if send:
        out_shape = jax.ShapeDtypeStruct((rows + 16, columns), BF16)
        out_specs = pl.BlockSpec((rows + 16, columns), lambda u, w: (0, 0))
    else:
        out_shape = (jax.ShapeDtypeStruct((n, rows, columns), F32), jax.ShapeDtypeStruct((n, 8, columns), F32))
        out_specs = [
            pl.BlockSpec((1, rows, columns), lambda u, w: (u, 0, 0)),
            pl.BlockSpec((1, 8, columns), lambda u, w: (u, 0, 0)),
        ]
    return pl.pallas_call(
        functools.partial(multiply, send=send),
        out_shape=out_shape,
        grid_spec=pltpu.PrefetchScalarGridSpec(
            num_scalar_prefetch=1,
            grid=(n,),
            in_specs=[
                pl.BlockSpec((1, rows, width), lambda u, w: (w[u], 0, 0)),
                pl.BlockSpec((1, rows, width), lambda u, w: (w[u], 0, 0)),
                pl.BlockSpec((2, 1, tiles, LANES), lambda u, w: (0, w[u], 0, 0)),
                pl.BlockSpec((2, 1, tiles, LANES), lambda u, w: (0, w[u], 0, 0)),
                pl.BlockSpec((1, columns, LANES), lambda u, w: (at, 0, 0)),
                pl.BlockSpec((1, columns, LANES), lambda u, w: (at, 0, 0)),
            ],
            out_specs=out_specs,
            scratch_shapes=[pltpu.VMEM((columns, 2 * width), BF16), pltpu.VMEM((columns, LANES), F32)],
        ),
        compiler_params=pltpu.CompilerParams(vmem_limit_bytes=24 << 20),
        cost_estimate=pl.CostEstimate(
            flops=n * rows * columns * width * 4, bytes_accessed=n * 6 << 20, transcendentals=n * columns * width * 2
        ),
        name="products",
    )(which, own, other, value, seam, low, shift)


def add_on(got_ref, product_ref, norm_ref, *out_refs):
    rows = product_ref.shape[1]
    each = product_ref.shape[2] // len(out_refs)
    for i, out_ref in enumerate(out_refs):
        at = slice(i * each, (i + 1) * each)
        out_ref[:rows, :] = (got_ref[:rows, at].astype(F32) + product_ref[0, :, at]).astype(BF16)
        norm = jnp.sum(got_ref[rows:, at].astype(F32), axis=0, keepdims=True) + norm_ref[0, :1, at]
        put_norm(out_ref, rows, slice(None), norm)


def added(got, product, norm, at, pieces):
    rows, columns = product.shape[1:]
    each = columns // pieces
    outs = [jax.ShapeDtypeStruct((rows + 16, each), BF16)] * pieces
    return pl.pallas_call(
        add_on,
        out_shape=outs,
        grid=(1,),
        in_specs=[
            pl.BlockSpec((rows + 16, columns), lambda i: (0, 0)),
            pl.BlockSpec((1, rows, columns), lambda i: (at, 0, 0)),
            pl.BlockSpec((1, 8, columns), lambda i: (at, 0, 0)),
        ],
        out_specs=[pl.BlockSpec((rows + 16, each), lambda i: (0, 0))] * pieces,
        compiler_params=pltpu.CompilerParams(vmem_limit_bytes=12 << 20),
        cost_estimate=pl.CostEstimate(flops=rows * columns * 1000, bytes_accessed=2 << 20, transcendentals=0),
        name="add_on",
    )(got, product, norm)


def finish(where_ref, a_ref, b_ref, c_ref, d_ref, product_ref, norm_ref, out_ref):
    rows = product_ref.shape[1]
    core = where_ref[0]
    squares = norm_ref[0, :1, :] + norm_ref[1, :1, :]
    for ref in (a_ref, b_ref, c_ref, d_ref):
        squares = squares + jnp.sum(ref[rows:, :].astype(F32), axis=0, keepdims=True)
    norm = jnp.sqrt(squares)
    for which, one, two in ((core, a_ref, d_ref), (1 - core, b_ref, c_ref)):
        total = product_ref[which] + one[:rows, :].astype(F32) + two[:rows, :].astype(F32)
        out_ref[which] = total / norm


def finished(where, first, second, first_across, second_across, product, norm):
    spec = pl.BlockSpec(memory_space=pltpu.VMEM)
    return pl.pallas_call(
        finish,
        out_shape=jax.ShapeDtypeStruct(product.shape, F32),
        in_specs=[pl.BlockSpec(memory_space=pltpu.SMEM)] + [spec] * 6,
        out_specs=spec,
        cost_estimate=pl.CostEstimate(flops=product.size * 100, bytes_accessed=4 << 20, transcendentals=0),
        compiler_params=pltpu.CompilerParams(vmem_limit_bytes=12 << 20),
        name="finish",
    )(where, first, second, first_across, second_across, product, norm)


def body(halves, spectrum, wanted, fraction):
    rows, width = halves.shape[1:]
    ncols = lax.axis_size("col")
    ndepth = lax.axis_size("depth")
    nrows = lax.axis_size(ROW)
    core = lax.axis_index("depth")
    col = lax.axis_index("col")
    place = lax.axis_index(ROW)
    share = wanted.shape[0] // ndepth
    reach = ncols // 2

    def along(core, col, by):
        return (col + (by if core == 0 else -by)) % ncols

    other = lax.ppermute(halves, "depth", [(0, 1), (1, 0)])

    mine = [
        spectrum.reshape(-1, LANES),
        lax.dynamic_slice_in_dim(wanted, core * share, share).astype(F32).reshape(-1, LANES),
        lax.dynamic_slice_in_dim(fraction, core * share, share).reshape(-1, LANES),
    ]
    root_row = mine[0].shape[0]
    seam_row = root_row + 8
    mine = jnp.concatenate(mine + [jnp.zeros((4, LANES), F32)], axis=0)
    pairs = []
    for r in range(nrows):
        for k in range(ncols):
            for c in range(ndepth):
                source = along(c, k, r // 2) * ndepth + (c ^ (r & 1))
                pairs.append((r * ncols * ndepth + source, r * ncols * ndepth + k * ndepth + c))
    theirs = lax.ppermute(mine, ROW + ("col", "depth"), pairs)
    last = place == nrows - 1
    seam = [jnp.where(last, h[0, rows - 1], h[1, 0]).astype(F32).reshape(-1, LANES) for h in (halves, other)]
    parcel = jnp.concatenate([theirs] + seam, axis=0)
    blocks = lax.all_to_all(jnp.broadcast_to(parcel[None], (nrows,) + parcel.shape), ROW, 0, 0, tiled=True)

    where = jnp.stack([core, col]).astype(jnp.int32)
    tiles = width // LANES
    value = blocks[:2, :root_row].reshape(2, 2, tiles, LANES)
    seam = jnp.stack(
        [blocks[nrows - 1, seam_row:].reshape(2, tiles, LANES), blocks[0, seam_row:].reshape(2, tiles, LANES)], axis=1
    )

    straight = [(k * ndepth + c, along(c, k, 1) * ndepth + c) for k in range(ncols) for c in range(ndepth)]
    across = [(k * ndepth + c, along(c, k, 1) * ndepth + 1 - c) for k in range(ncols) for c in range(ndepth)]
    ring = ("col", "depth")
    first = core.astype(jnp.int32)
    one = jnp.stack([first])
    two = jnp.stack([1 - first])
    both = jnp.stack([1 - first, first])

    multiplied = functools.partial(products, own=halves, other=other, value=value, seam=seam)
    low, shift = roots_of(where, blocks, (reach,), root_row)
    a = multiplied(one, low=low, shift=shift, at=0, columns=2 * share, send=True)
    a = lax.ppermute(a, ring, straight)
    low, shift = roots_of(where, blocks, tuple(range(reach - 1, -1, -1)), root_row)
    b = multiplied(two, low=low, shift=shift, at=0, columns=2 * share, send=True)
    b = lax.ppermute(b, ring, straight)
    product, norm = multiplied(one, low=low, shift=shift, at=0, columns=2 * share, send=False)
    (a,) = added(a, product, norm, 0, 1)
    for step in range(reach - 2, 0, -1):
        a = lax.ppermute(a, ring, straight)
        product, norm = multiplied(both, low=low, shift=shift, at=reach - 1 - step, columns=2 * share, send=False)
        if step > 1:
            (b,) = added(b, product, norm, 0, 1)
            b = lax.ppermute(b, ring, straight)
            (a,) = added(a, product, norm, 1, 1)
        else:
            b, b_across = added(b, product, norm, 0, 2)
            b = lax.ppermute(b, ring, straight)
            b_across = lax.ppermute(b_across, ring, across)
            a, a_across = added(a, product, norm, 1, 2)
    a = lax.ppermute(a, ring, straight)
    a_across = lax.ppermute(a_across, ring, across)
    product, norm = multiplied(
        jnp.arange(2, dtype=jnp.int32), low=low, shift=shift, at=reach - 1, columns=share, send=False
    )
    return finished(where, a, b, a_across, b_across, product, norm)


def solution(mesh):
    split = Mesh(
        mesh.devices.reshape(4, 4, mesh.shape["col"], mesh.shape["depth"]), ("row_0", "row_1", "col", "depth")
    )
    in_specs = (P(None, ROW, ("col", "depth")), P(None, ("col", "depth")), P("col"), P("col"))
    out_specs = P(None, ROW, ("col", "depth"))
    return jax.shard_map(body, mesh=split, in_specs=in_specs, out_specs=out_specs, check_vma=False)
```

```python
import functools

import jax
import jax.numpy as jnp
from jax import lax
from jax.experimental import pallas as pl
from jax.experimental.pallas import tpu as pltpu
from jax.sharding import Mesh
from jax.sharding import PartitionSpec as P


ROW = ("row_0", "row_1")
LANES = 128
PIECE = 64
F32 = jnp.float32
BF16 = jnp.bfloat16


def look_up(core, col, blocks_ref, low_ref, shift_ref, *, step, value_rows, columns):
    count = blocks_ref.shape[0]
    table = blocks_ref[:, :value_rows, :].reshape(count * value_rows, LANES)
    high = table.astype(BF16)
    rest = table - high.astype(F32)
    middle = rest.astype(BF16)
    small = (rest - middle.astype(F32)).astype(BF16)
    split = jnp.concatenate([high, middle, small], axis=1)
    per_block = value_rows * LANES
    half = per_block // 2

    roots = blocks_ref[2 * step, value_rows : value_rows + 8, :]
    swapped = jnp.concatenate([roots[2:4], roots[0:2], roots[6:8], roots[4:6]], axis=0)
    roots = jnp.where(core == 0, roots, swapped)
    wanted = roots[:4].astype(jnp.int32)
    rows = []
    for position in (wanted, wanted + 1):
        owner = lax.shift_right_logical(position, per_block.bit_length() - 1)
        ahead = lax.shift_right_logical(owner, 1) - col
        ahead = jnp.where(core == 0, ahead, -ahead) & (count // 2 - 1)
        order = ahead * 2 + ((owner & 1) ^ core)
        inside = position & (per_block - 1)
        index = (inside & 1) * half + lax.shift_right_logical(inside, 1)
        rows += [order * value_rows + lax.shift_right_logical(index, 7), index & (LANES - 1)]
    rows = jnp.concatenate([r.astype(F32) for r in rows] + [roots[4:], jnp.zeros((LANES - 20, LANES), F32)], axis=0)
    spots = jnp.transpose(rows)
    row_ids = lax.broadcasted_iota(jnp.int32, (LANES, count * value_rows), 1).astype(F32)
    lane_ids = lax.broadcasted_iota(jnp.int32, (LANES, LANES), 1).astype(F32)
    for tile in range(columns // LANES):
        picks = [jnp.where(row_ids == spots[:, k + tile : k + tile + 1], 1.0, 0.0).astype(BF16) for k in (0, 8)]
        got = jnp.dot(jnp.concatenate(picks, axis=0), split, preferred_element_type=F32)
        got = (got[:, :LANES] + got[:, LANES : 2 * LANES]) + got[:, 2 * LANES :]
        lower, upper = (
            jnp.sum(jnp.where(lane_ids == spots[:, k + tile : k + tile + 1], got[at : at + LANES], 0.0), axis=1, keepdims=True)
            for k, at in ((4, 0), (12, LANES))
        )
        shift = spots[:, 16 + tile : 17 + tile] * (upper - lower)
        at = slice(tile * LANES, (tile + 1) * LANES)
        low_ref[at, :] = jnp.broadcast_to(lower, (LANES, LANES))
        shift_ref[at, :] = jnp.broadcast_to(shift, (LANES, LANES))


def multiply(which_ref, where_ref, blocks_ref, own_ref, other_ref, *refs, step, sends, tall):
    out_ref, norm_ref = refs[0], refs[1] if len(refs) > 7 else None
    low_ref, shift_ref, block_ref, square_ref, halves_ref, sems = refs[-6:]
    unit = pl.program_id(0)
    units = halves_ref.shape[0]
    columns = low_ref.shape[0]
    rows, width = halves_ref.shape[2:]
    tiles = width // LANES
    value_rows = 2 * tiles
    half = which_ref[unit]
    last = jnp.where(half == 0, blocks_ref.shape[0] - 1, 0)

    def load(u, source):
        ref = (own_ref, other_ref)[source]
        return pltpu.make_async_copy(ref.at[which_ref[u]], halves_ref.at[u, source], sems.at[u, source])

    @pl.when(unit == 0)
    def _():
        for u in range(units):
            for source in range(2):
                load(u, source).start()
        look_up(
            where_ref[0], where_ref[1], blocks_ref, low_ref, shift_ref, step=step, value_rows=value_rows, columns=columns
        )

    values = [[blocks_ref[s, pl.ds(half * tiles + t, 1), :] for t in range(tiles)] for s in range(2)]
    seams = [[blocks_ref[last, value_rows + 8 + s * tiles + t, :][None] for t in range(tiles)] for s in range(2)]
    for part in range(columns // 256):
        for piece in range(256 // PIECE):
            start = part * 256 + piece * PIECE
            low = low_ref[start : start + PIECE, :]
            shift = shift_ref[start : start + PIECE, :]
            square = jnp.zeros((PIECE, LANES), F32)
            for source in range(2):
                for tile in range(tiles):
                    cauchy = seams[source][tile] / ((values[source][tile] - low) - shift)
                    square = square + cauchy * cauchy
                    block_ref[
                        start : start + PIECE, source * width + tile * LANES : source * width + (tile + 1) * LANES
                    ] = cauchy.astype(BF16)
            square_ref[start : start + PIECE, :] = square
        if part == 0:
            for source in range(2):
                load(unit, source).wait()
        at = slice(part * 256, (part + 1) * 256)
        nt = (((1,), (1,)), ((), ()))
        product = lax.dot_general(halves_ref[unit, 0], block_ref[at, :width], nt, preferred_element_type=F32)
        product = product + lax.dot_general(halves_ref[unit, 1], block_ref[at, width:], nt, preferred_element_type=F32)
        norm = jnp.sum(jnp.transpose(square_ref[at, :]), axis=0, keepdims=True)
        if sends:
            out_ref[:rows, at] = product.astype(BF16)
        else:
            out_ref[0, :, at] = product
        if tall:
            put_norm(out_ref, rows, at, norm)
        else:
            norm_ref[:, at] = jnp.where(unit == 0, 0.0, norm_ref[:, at]) + jnp.broadcast_to(norm, (8, 256))


def put_norm(out_ref, rows, at, norm):
    high = norm.astype(BF16).astype(F32)
    row = lax.broadcasted_iota(jnp.int32, (16, norm.shape[1]), 0)
    both = jnp.where(row == 0, high, jnp.where(row == 1, norm - high, 0.0))
    out_ref[rows : rows + 16, at] = both.astype(BF16)


def products(which, where, blocks, own, other, step, columns, sends=False, tall=False):
    n = which.shape[0]
    rows, width = own.shape[1:]
    if sends:
        height = rows + 16 if tall else rows
        out_shape = [jax.ShapeDtypeStruct((height, columns), BF16)]
        out_specs = [pl.BlockSpec((height, columns), lambda u, w: (0, 0))]
    else:
        out_shape = [jax.ShapeDtypeStruct((n, rows, columns), F32)]
        out_specs = [pl.BlockSpec((1, rows, columns), lambda u, w: (u, 0, 0))]
    if not tall:
        out_shape.append(jax.ShapeDtypeStruct((8, columns), F32))
        out_specs.append(pl.BlockSpec((8, columns), lambda u, w: (0, 0)))
    return pl.pallas_call(
        functools.partial(multiply, step=step, sends=sends, tall=tall),
        out_shape=out_shape,
        grid_spec=pltpu.PrefetchScalarGridSpec(
            num_scalar_prefetch=1,
            grid=(n,),
            in_specs=[
                pl.BlockSpec(memory_space=pltpu.SMEM),
                pl.BlockSpec(blocks.shape, lambda u, w: (0, 0, 0)),
                pl.BlockSpec(memory_space=pltpu.HBM),
                pl.BlockSpec(memory_space=pltpu.HBM),
            ],
            out_specs=out_specs,
            scratch_shapes=[
                pltpu.VMEM((columns, LANES), F32),
                pltpu.VMEM((columns, LANES), F32),
                pltpu.VMEM((columns, 2 * width), BF16),
                pltpu.VMEM((columns, LANES), F32),
                pltpu.VMEM((n, 2, rows, width), BF16),
                pltpu.SemaphoreType.DMA((n, 2)),
            ],
        ),
        compiler_params=pltpu.CompilerParams(vmem_limit_bytes=52 << 20),
        cost_estimate=pl.CostEstimate(
            flops=n * rows * columns * width * 4, bytes_accessed=n * 6 << 20, transcendentals=n * columns * width * 2
        ),
        name="products",
    )(which, where, blocks, own, other)


def add_on(got_ref, product_ref, norm_ref, *out_refs):
    rows = product_ref.shape[1]
    each = product_ref.shape[2] // len(out_refs)
    for i, out_ref in enumerate(out_refs):
        at = slice(i * each, (i + 1) * each)
        out_ref[:rows, :] = (got_ref[:rows, at].astype(F32) + product_ref[0, :, at]).astype(BF16)
        if out_ref.shape[0] > rows:
            norm = jnp.sum(got_ref[rows:, at].astype(F32), axis=0, keepdims=True) + norm_ref[:1, at]
            put_norm(out_ref, rows, slice(None), norm)


def added(got, product, norm, at, pieces):
    rows, columns = product.shape[1:]
    each = columns // pieces
    tall = got.shape[0]
    outs = [jax.ShapeDtypeStruct((tall, each), BF16)] * pieces
    return pl.pallas_call(
        add_on,
        out_shape=outs,
        grid=(1,),
        in_specs=[
            pl.BlockSpec((tall, columns), lambda i: (0, 0)),
            pl.BlockSpec((1, rows, columns), lambda i: (at, 0, 0)),
            pl.BlockSpec((8, columns), lambda i: (0, 0)),
        ],
        out_specs=[pl.BlockSpec((tall, each), lambda i: (0, 0))] * pieces,
        compiler_params=pltpu.CompilerParams(vmem_limit_bytes=8 << 20),
        cost_estimate=pl.CostEstimate(flops=rows * columns * 1000, bytes_accessed=2 << 20, transcendentals=0),
        name="add_on",
    )(got, product, norm)


def finish(which_ref, a_ref, b_ref, c_ref, d_ref, product_ref, norm_ref, out_ref):
    rows = product_ref.shape[1]
    squares = norm_ref[:1, :]
    for ref in (a_ref, c_ref):
        squares = squares + jnp.sum(ref[rows:, :].astype(F32), axis=0, keepdims=True)
    norm = jnp.sqrt(squares)
    for unit, (one, two) in enumerate(((a_ref, d_ref), (b_ref, c_ref))):

        @pl.when(pl.program_id(0) == unit)
        def _():
            total = product_ref[0] + one[:rows, :].astype(F32) + two[:rows, :].astype(F32)
            out_ref[0] = total / norm


def finished(which, first, second, first_across, second_across, product, norm):
    n, rows, columns = product.shape
    whole = [pl.BlockSpec(x.shape, lambda u, w: (0, 0)) for x in (first, second, first_across, second_across)]
    return pl.pallas_call(
        finish,
        out_shape=jax.ShapeDtypeStruct(product.shape, F32),
        grid_spec=pltpu.PrefetchScalarGridSpec(
            num_scalar_prefetch=1,
            grid=(n,),
            in_specs=whole
            + [pl.BlockSpec((1, rows, columns), lambda u, w: (w[u], 0, 0)), pl.BlockSpec(norm.shape, lambda u, w: (0, 0))],
            out_specs=pl.BlockSpec((1, rows, columns), lambda u, w: (w[u], 0, 0)),
        ),
        cost_estimate=pl.CostEstimate(flops=product.size * 100, bytes_accessed=4 << 20, transcendentals=0),
        compiler_params=pltpu.CompilerParams(vmem_limit_bytes=8 << 20),
        name="finish",
    )(which, first, second, first_across, second_across, product, norm)


def body(halves, spectrum, wanted, fraction):
    rows, _ = halves.shape[1:]
    ncols = lax.axis_size("col")
    ndepth = lax.axis_size("depth")
    nrows = lax.axis_size(ROW)
    core = lax.axis_index("depth").astype(jnp.int32)
    col = lax.axis_index("col").astype(jnp.int32)
    place = lax.axis_index(ROW)
    columns = wanted.shape[0]
    reach = ncols // 2

    def along(core, col, by):
        return (col + (by if core == 0 else -by)) % ncols

    pairs = []
    for r in range(nrows):
        for k in range(ncols):
            for c in range(ndepth):
                source = along(c, k, r // 2) * ndepth + (c ^ (r & 1))
                pairs.append((r * ncols * ndepth + source, r * ncols * ndepth + k * ndepth + c))
    theirs = [lax.ppermute(x, ROW + ("col", "depth"), pairs) for x in (spectrum, wanted, fraction)]
    other = lax.ppermute(halves, "depth", [(0, 1), (1, 0)])
    last = place == nrows - 1
    seam = [jnp.where(last, h[0, rows - 1], h[1, 0]) for h in (halves, other)]
    parcel = jnp.concatenate([x.astype(F32).reshape(-1, LANES) for x in theirs + seam], axis=0)
    blocks = lax.all_to_all(jnp.broadcast_to(parcel[None], (nrows,) + parcel.shape), ROW, 0, 0, tiled=True)

    straight = [(k * ndepth + c, along(c, k, 1) * ndepth + c) for k in range(ncols) for c in range(ndepth)]
    across = [(k * ndepth + c, along(c, k, 1) * ndepth + 1 - c) for k in range(ncols) for c in range(ndepth)]
    ring = ("col", "depth")
    where = jnp.stack([core, col])
    both = jnp.stack([1 - core, core])
    multiplied = functools.partial(products, where=where, blocks=blocks, own=halves, other=other)

    (a,) = multiplied(both[1:], step=reach, columns=columns, sends=True, tall=True)
    a = lax.ppermute(a, ring, straight)
    b, norm = multiplied(both[:1], step=reach - 1, columns=columns, sends=True)
    b = lax.ppermute(b, ring, straight)
    product, more = multiplied(both[1:], step=reach - 1, columns=columns)
    (a,) = added(a, product, norm + more, 0, 1)
    for step in range(reach - 2, 0, -1):
        a = lax.ppermute(a, ring, straight)
        product, norm = multiplied(both[:1], step=step, columns=columns)
        pieces = 1 if step > 1 else 2
        b, *b_across = added(b, product, norm, 0, pieces)
        b = lax.ppermute(b, ring, straight)
        b_across = [lax.ppermute(x, ring, across) for x in b_across]
        product, more = multiplied(both[1:], step=step, columns=columns)
        a, *a_across = added(a, product, norm + more, 0, pieces)
    a = lax.ppermute(a, ring, straight)
    a_across = [lax.ppermute(x, ring, across) for x in a_across]
    product, norm = multiplied(jnp.arange(2, dtype=jnp.int32), step=0, columns=columns // ndepth)
    return finished(both[::-1], a, b, a_across[0], b_across[0], product, norm)


def solution(mesh):
    split = Mesh(
        mesh.devices.reshape(4, 4, mesh.shape["col"], mesh.shape["depth"]), ("row_0", "row_1", "col", "depth")
    )
    in_specs = (P(None, ROW, ("col", "depth")), P(None, ("col", "depth")), P("col"), P("col"))
    out_specs = P(None, ROW, ("col", "depth"))
    return jax.shard_map(body, mesh=split, in_specs=in_specs, out_specs=out_specs, check_vma=False)
```

```python
import functools

import jax
import jax.numpy as jnp
from jax import lax
from jax.experimental import pallas as pl
from jax.experimental.pallas import tpu as pltpu
from jax.sharding import Mesh
from jax.sharding import PartitionSpec as P


ROW = ("row_0", "row_1")
LANES = 128
PIECE = 64
F32 = jnp.float32
BF16 = jnp.bfloat16


def heading(step):
    core = lax.axis_index("depth").astype(jnp.int32)
    col = lax.axis_index("col").astype(jnp.int32)
    ncols = lax.axis_size("col")
    target = lax.rem(col + jnp.where(core == 0, step, ncols - step), ncols)
    return core, col, target


def look_up(core, target, blocks_ref, low_ref, shift_ref, *, value_rows, first, count):
    places = blocks_ref.shape[0]
    table = blocks_ref[:, :value_rows, :].reshape(places * value_rows, LANES)
    high = table.astype(BF16)
    rest = table - high.astype(F32)
    middle = rest.astype(BF16)
    small = (rest - middle.astype(F32)).astype(BF16)
    split = jnp.concatenate([high, middle, small], axis=1)
    per_block = value_rows * LANES
    half = per_block // 2

    roots = blocks_ref[2 * target, value_rows : value_rows + 8, :]
    swapped = jnp.concatenate([roots[2:4], roots[0:2], roots[6:8], roots[4:6]], axis=0)
    roots = jnp.where(core == 0, roots, swapped)
    wanted = roots[:4].astype(jnp.int32)
    rows = []
    for position in (wanted, wanted + 1):
        owner = lax.shift_right_logical(position, per_block.bit_length() - 1)
        inside = position & (per_block - 1)
        index = (inside & 1) * half + lax.shift_right_logical(inside, 1)
        rows += [owner * value_rows + lax.shift_right_logical(index, 7), index & (LANES - 1)]
    rows = jnp.concatenate([r.astype(F32) for r in rows] + [roots[4:], jnp.zeros((LANES - 20, LANES), F32)], axis=0)
    spots = jnp.transpose(rows)
    row_ids = lax.broadcasted_iota(jnp.int32, (LANES, places * value_rows), 1).astype(F32)
    lane_ids = lax.broadcasted_iota(jnp.int32, (LANES, LANES), 1).astype(F32)
    for tile in range(first, first + count):
        picks = [jnp.where(row_ids == spots[:, k + tile : k + tile + 1], 1.0, 0.0).astype(BF16) for k in (0, 8)]
        got = jnp.dot(jnp.concatenate(picks, axis=0), split, preferred_element_type=F32)
        got = (got[:, :LANES] + got[:, LANES : 2 * LANES]) + got[:, 2 * LANES :]
        lower, upper = (
            jnp.sum(jnp.where(lane_ids == spots[:, k + tile : k + tile + 1], got[at : at + LANES], 0.0), axis=1, keepdims=True)
            for k, at in ((4, 0), (12, LANES))
        )
        shift = spots[:, 16 + tile : 17 + tile] * (upper - lower)
        at = slice((tile - first) * LANES, (tile - first + 1) * LANES)
        low_ref[at, :] = jnp.broadcast_to(lower, (LANES, LANES))
        shift_ref[at, :] = jnp.broadcast_to(shift, (LANES, LANES))


def multiply(blocks_ref, seam_ref, own_ref, other_ref, *refs, step, which, first, sends, tall):
    out_ref, norm_ref = refs[0], None if tall else refs[1]
    low_ref, shift_ref, block_ref, square_ref, halves_ref, sems = refs[-6:]
    columns = low_ref.shape[0]
    rows, width = halves_ref.shape[2:]
    tiles = width // LANES
    value_rows = 2 * tiles
    core, col, target = heading(step)
    halves = [core if w == "first" else 1 - core if w == "second" else w for w in which]
    loads = [
        [
            pltpu.make_async_copy(ref.at[half], halves_ref.at[u, source], sems.at[u, source])
            for source, ref in enumerate((own_ref, other_ref))
        ]
        for u, half in enumerate(halves)
    ]
    for pair in loads:
        for load in pair:
            load.start()
    look_up(core, target, blocks_ref, low_ref, shift_ref, value_rows=value_rows, first=first, count=columns // LANES)
    here = [2 * col + core, 2 * col + 1 - core]
    for u, half in enumerate(halves):
        values = [[blocks_ref[s, pl.ds(half * tiles + t, 1), :] for t in range(tiles)] for s in here]
        rows_of = seam_ref[jnp.where(half == 0, seam_ref.shape[0] - 1, 0)].astype(F32)
        seams = [[rows_of[s * tiles + t : s * tiles + t + 1] for t in range(tiles)] for s in range(2)]
        for part in range(columns // 256):
            for piece in range(256 // PIECE):
                start = part * 256 + piece * PIECE
                low = low_ref[start : start + PIECE, :]
                shift = shift_ref[start : start + PIECE, :]
                square = jnp.zeros((PIECE, LANES), F32)
                for source in range(2):
                    for tile in range(tiles):
                        cauchy = seams[source][tile] / ((values[source][tile] - low) - shift)
                        square = square + cauchy * cauchy
                        block_ref[
                            start : start + PIECE, source * width + tile * LANES : source * width + (tile + 1) * LANES
                        ] = cauchy.astype(BF16)
                square_ref[start : start + PIECE, :] = square
            if part == 0:
                for load in loads[u]:
                    load.wait()
            at = slice(part * 256, (part + 1) * 256)
            nt = (((1,), (1,)), ((), ()))
            product = lax.dot_general(halves_ref[u, 0], block_ref[at, :width], nt, preferred_element_type=F32)
            product = product + lax.dot_general(halves_ref[u, 1], block_ref[at, width:], nt, preferred_element_type=F32)
            norm = jnp.sum(jnp.transpose(square_ref[at, :]), axis=0, keepdims=True)
            if sends:
                out_ref[:rows, at] = product.astype(BF16)
            else:
                out_ref[u, :, at] = product
            if tall:
                put_norm(out_ref, rows, at, norm)
            elif u == 0:
                norm_ref[:, at] = jnp.broadcast_to(norm, (8, 256))
            else:
                norm_ref[:, at] += jnp.broadcast_to(norm, (8, 256))


def put_norm(out_ref, rows, at, norm):
    high = norm.astype(BF16).astype(F32)
    row = lax.broadcasted_iota(jnp.int32, (16, norm.shape[1]), 0)
    both = jnp.where(row == 0, high, jnp.where(row == 1, norm - high, 0.0))
    out_ref[rows : rows + 16, at] = both.astype(BF16)


VMEM = pl.BlockSpec(memory_space=pltpu.VMEM)
HBM = pl.BlockSpec(memory_space=pl.ANY)


def products(which, blocks, seam, own, other, step, columns, first=0, sends=False, tall=False):
    n = len(which)
    rows, width = own.shape[1:]
    if sends:
        out_shape = [jax.ShapeDtypeStruct((rows + 16 if tall else rows, columns), BF16)]
    else:
        out_shape = [jax.ShapeDtypeStruct((n, rows, columns), F32)]
    if not tall:
        out_shape.append(jax.ShapeDtypeStruct((8, columns), F32))
    return pl.pallas_call(
        functools.partial(multiply, step=step, which=which, first=first, sends=sends, tall=tall),
        out_shape=out_shape,
        in_specs=[VMEM, VMEM, HBM, HBM],
        out_specs=[VMEM] * len(out_shape),
        scratch_shapes=[
            pltpu.VMEM((columns, LANES), F32),
            pltpu.VMEM((columns, LANES), F32),
            pltpu.VMEM((columns, 2 * width), BF16),
            pltpu.VMEM((columns, LANES), F32),
            pltpu.VMEM((n, 2, rows, width), BF16),
            pltpu.SemaphoreType.DMA((n, 2)),
        ],
        compiler_params=pltpu.CompilerParams(vmem_limit_bytes=52 << 20),
        cost_estimate=pl.CostEstimate(
            flops=n * rows * columns * width * 4, bytes_accessed=n * 6 << 20, transcendentals=n * columns * width * 2
        ),
        name="products",
    )(blocks, seam, own, other)


def add_on(got_ref, product_ref, norm_ref, *out_refs):
    rows = product_ref.shape[1]
    each = product_ref.shape[2] // len(out_refs)
    for i, out_ref in enumerate(out_refs):
        at = slice(i * each, (i + 1) * each)
        out_ref[:rows, :] = (got_ref[:rows, at].astype(F32) + product_ref[0, :, at]).astype(BF16)
        if out_ref.shape[0] > rows:
            norm = jnp.sum(got_ref[rows:, at].astype(F32), axis=0, keepdims=True) + norm_ref[:1, at]
            put_norm(out_ref, rows, slice(None), norm)


def added(got, product, norm, pieces):
    rows, columns = product.shape[1:]
    return pl.pallas_call(
        add_on,
        out_shape=[jax.ShapeDtypeStruct((got.shape[0], columns // pieces), BF16)] * pieces,
        in_specs=[VMEM] * 3,
        out_specs=[VMEM] * pieces,
        compiler_params=pltpu.CompilerParams(vmem_limit_bytes=8 << 20),
        cost_estimate=pl.CostEstimate(flops=rows * columns * 1000, bytes_accessed=2 << 20, transcendentals=0),
        name="add_on",
    )(got, product, norm)


def finish(a_ref, b_ref, c_ref, d_ref, product_ref, norm_ref, out_ref, held_ref, sems):
    rows = product_ref.shape[1]
    step = rows // 2
    squares = norm_ref[:1, :]
    for ref in (a_ref, c_ref):
        squares = squares + jnp.sum(ref[rows:, :].astype(F32), axis=0, keepdims=True)
    norm = jnp.sqrt(squares)
    core = lax.axis_index("depth").astype(jnp.int32)
    stores = []
    for half, one, two in ((core, a_ref, d_ref), (1 - core, b_ref, c_ref)):
        for start in range(0, rows, step):
            at = pl.ds(start, step)
            total = product_ref[half, at] + one[at, :].astype(F32) + two[at, :].astype(F32)
            held_ref[len(stores)] = total / norm
            store = pltpu.make_async_copy(held_ref.at[len(stores)], out_ref.at[half, at], sems.at[len(stores)])
            store.start()
            stores.append(store)
    for store in stores:
        store.wait()


def finished(first, second, first_across, second_across, product, norm):
    _, rows, columns = product.shape
    return pl.pallas_call(
        finish,
        out_shape=jax.ShapeDtypeStruct(product.shape, F32),
        in_specs=[VMEM] * 6,
        out_specs=HBM,
        scratch_shapes=[pltpu.VMEM((4, rows // 2, columns), F32), pltpu.SemaphoreType.DMA((4,))],
        cost_estimate=pl.CostEstimate(flops=product.size * 100, bytes_accessed=4 << 20, transcendentals=0),
        compiler_params=pltpu.CompilerParams(vmem_limit_bytes=8 << 20),
        name="finish",
    )(first, second, first_across, second_across, product, norm)


def pack(spectrum_ref, wanted_ref, fraction_ref, out_ref):
    rows = []
    for half in range(2):
        for start in range(0, spectrum_ref.shape[1], LANES):
            rows.append(spectrum_ref[half : half + 1, start : start + LANES])
    for ref in (wanted_ref, fraction_ref):
        for start in range(0, ref.shape[1], LANES):
            rows.append(ref[:, start : start + LANES].astype(F32))
    out_ref[...] = jnp.broadcast_to(jnp.concatenate(rows, axis=0)[None], out_ref.shape)


def packed(spectrum, wanted, fraction, copies):
    rows = (spectrum.size + wanted.size + fraction.size) // LANES
    return pl.pallas_call(
        pack,
        out_shape=jax.ShapeDtypeStruct((copies, rows, LANES), F32),
        in_specs=[VMEM] * 3,
        out_specs=VMEM,
        compiler_params=pltpu.CompilerParams(vmem_limit_bytes=4 << 20),
        cost_estimate=pl.CostEstimate(flops=1000, bytes_accessed=400000, transcendentals=0),
        name="pack",
    )(spectrum, wanted.reshape(1, -1), fraction.reshape(1, -1))


def body(halves, spectrum, wanted, fraction):
    rows = halves.shape[1]
    ncols = lax.axis_size("col")
    ndepth = lax.axis_size("depth")
    nrows = lax.axis_size(ROW)
    columns = wanted.shape[0]
    reach = ncols // 2
    ring = ("col", "depth")

    def along(core, col, by):
        return (col + (by if core == 0 else -by)) % ncols

    straight = [(k * ndepth + c, along(c, k, 1) * ndepth + c) for k in range(ncols) for c in range(ndepth)]
    across = [(k * ndepth + c, along(c, k, 1) * ndepth + 1 - c) for k in range(ncols) for c in range(ndepth)]

    other = lax.ppermute(halves, "depth", [(0, 1), (1, 0)])
    blocks = lax.all_to_all(packed(spectrum, wanted, fraction, ncols * ndepth), ring, 0, 0, tiled=True)
    last = lax.axis_index(ROW) == nrows - 1
    seam = [jnp.where(last, h[0, rows - 1], h[1, 0]).reshape(-1, LANES) for h in (halves, other)]
    seam = jnp.concatenate(seam, axis=0)
    seam = lax.all_to_all(jnp.broadcast_to(seam[None], (nrows,) + seam.shape), ROW, 0, 0, tiled=True)

    multiplied = functools.partial(products, blocks=blocks, seam=seam, own=halves, other=other, columns=columns)
    (a,) = multiplied(("first",), step=reach, sends=True, tall=True)
    a = lax.ppermute(a, ring, straight)
    b, norm = multiplied(("second",), step=reach - 1, sends=True)
    b = lax.ppermute(b, ring, straight)
    product, more = multiplied(("first",), step=reach - 1)
    (a,) = added(a, product, norm + more, 1)
    for step in range(reach - 2, 0, -1):
        a = lax.ppermute(a, ring, straight)
        product, norm = multiplied(("second",), step=step)
        pieces = 1 if step > 1 else 2
        b, *b_across = added(b, product, norm, pieces)
        b = lax.ppermute(b, ring, straight)
        b_across = [lax.ppermute(x, ring, across) for x in b_across]
        product, more = multiplied(("first",), step=step)
        a, *a_across = added(a, product, norm + more, pieces)
    a = lax.ppermute(a, ring, straight)
    a_across = [lax.ppermute(x, ring, across) for x in a_across]
    product, norm = multiplied((0, 1), step=0, columns=columns // ndepth)
    return finished(a, b, a_across[0], b_across[0], product, norm)


def solution(mesh):
    split = Mesh(
        mesh.devices.reshape(4, 4, mesh.shape["col"], mesh.shape["depth"]), ("row_0", "row_1", "col", "depth")
    )
    in_specs = (P(None, ROW, ("col", "depth")), P(None, ("col", "depth")), P("col"), P("col"))
    out_specs = P(None, ROW, ("col", "depth"))
    return jax.shard_map(body, mesh=split, in_specs=in_specs, out_specs=out_specs, check_vma=False)
```

```python
import functools

import jax
import jax.numpy as jnp
from jax import lax
from jax.experimental import pallas as pl
from jax.experimental.pallas import tpu as pltpu
from jax.sharding import Mesh
from jax.sharding import PartitionSpec as P


ROW = ("row_0", "row_1")
LANES = 128
PIECE = 64
F32 = jnp.float32
BF16 = jnp.bfloat16


def look_up(core, col, blocks_ref, low_ref, shift_ref, *, step, value_rows, first, count):
    places = blocks_ref.shape[0]
    table = blocks_ref[:, :value_rows, :].reshape(places * value_rows, LANES)
    high = table.astype(BF16)
    rest = table - high.astype(F32)
    middle = rest.astype(BF16)
    small = (rest - middle.astype(F32)).astype(BF16)
    split = jnp.concatenate([high, middle, small], axis=1)
    per_block = value_rows * LANES
    half = per_block // 2

    roots = blocks_ref[2 * step, value_rows : value_rows + 8, :]
    swapped = jnp.concatenate([roots[2:4], roots[0:2], roots[6:8], roots[4:6]], axis=0)
    roots = jnp.where(core == 0, roots, swapped)
    wanted = roots[:4].astype(jnp.int32)
    rows = []
    for position in (wanted, wanted + 1):
        owner = lax.shift_right_logical(position, per_block.bit_length() - 1)
        ahead = lax.shift_right_logical(owner, 1) - col
        ahead = jnp.where(core == 0, ahead, -ahead) & (places // 2 - 1)
        owner = ahead * 2 + ((owner & 1) ^ core)
        inside = position & (per_block - 1)
        index = (inside & 1) * half + lax.shift_right_logical(inside, 1)
        rows += [owner * value_rows + lax.shift_right_logical(index, 7), index & (LANES - 1)]
    rows = jnp.concatenate([r.astype(F32) for r in rows] + [roots[4:], jnp.zeros((LANES - 20, LANES), F32)], axis=0)
    spots = jnp.transpose(rows)
    row_ids = lax.broadcasted_iota(jnp.int32, (LANES, places * value_rows), 1).astype(F32)
    lane_ids = lax.broadcasted_iota(jnp.int32, (LANES, LANES), 1).astype(F32)
    for tile in range(first, first + count):
        picks = [jnp.where(row_ids == spots[:, k + tile : k + tile + 1], 1.0, 0.0).astype(BF16) for k in (0, 8)]
        got = jnp.dot(jnp.concatenate(picks, axis=0), split, preferred_element_type=F32)
        got = (got[:, :LANES] + got[:, LANES : 2 * LANES]) + got[:, 2 * LANES :]
        lower, upper = (
            jnp.sum(jnp.where(lane_ids == spots[:, k + tile : k + tile + 1], got[at : at + LANES], 0.0), axis=1, keepdims=True)
            for k, at in ((4, 0), (12, LANES))
        )
        shift = spots[:, 16 + tile : 17 + tile] * (upper - lower)
        at = slice((tile - first) * LANES, (tile - first + 1) * LANES)
        low_ref[at, :] = jnp.broadcast_to(lower, (LANES, LANES))
        shift_ref[at, :] = jnp.broadcast_to(shift, (LANES, LANES))


def multiply(blocks_ref, own_ref, other_ref, *refs, step, which, first, sends, tall):
    out_ref, norm_ref = refs[0], None if tall else refs[1]
    low_ref, shift_ref, block_ref, square_ref, halves_ref, sems = refs[-6:]
    columns = low_ref.shape[0]
    rows, width = halves_ref.shape[2:]
    tiles = width // LANES
    value_rows = 2 * tiles
    core = lax.axis_index("depth").astype(jnp.int32)
    col = lax.axis_index("col").astype(jnp.int32)
    halves = [core if w == "first" else 1 - core if w == "second" else w for w in which]
    loads = [
        [
            pltpu.make_async_copy(ref.at[half], halves_ref.at[u, source], sems.at[u, source])
            for source, ref in enumerate((own_ref, other_ref))
        ]
        for u, half in enumerate(halves)
    ]
    for pair in loads:
        for load in pair:
            load.start()
    look_up(
        core, col, blocks_ref, low_ref, shift_ref, step=step, value_rows=value_rows, first=first, count=columns // LANES
    )
    for u, half in enumerate(halves):
        values = [[blocks_ref[s, pl.ds(half * tiles + t, 1), :] for t in range(tiles)] for s in range(2)]
        edge = blocks_ref[jnp.where(half == 0, blocks_ref.shape[0] - 1, 0), value_rows + 8 :, :]
        seams = [[edge[s * tiles + t : s * tiles + t + 1] for t in range(tiles)] for s in range(2)]
        for part in range(columns // 256):
            for piece in range(256 // PIECE):
                start = part * 256 + piece * PIECE
                low = low_ref[start : start + PIECE, :]
                shift = shift_ref[start : start + PIECE, :]
                square = jnp.zeros((PIECE, LANES), F32)
                for source in range(2):
                    for tile in range(tiles):
                        cauchy = seams[source][tile] / ((values[source][tile] - low) - shift)
                        square = square + cauchy * cauchy
                        block_ref[
                            start : start + PIECE, source * width + tile * LANES : source * width + (tile + 1) * LANES
                        ] = cauchy.astype(BF16)
                square_ref[start : start + PIECE, :] = square
            if part == 0:
                for load in loads[u]:
                    load.wait()
            at = slice(part * 256, (part + 1) * 256)
            nt = (((1,), (1,)), ((), ()))
            product = lax.dot_general(halves_ref[u, 0], block_ref[at, :width], nt, preferred_element_type=F32)
            product = product + lax.dot_general(halves_ref[u, 1], block_ref[at, width:], nt, preferred_element_type=F32)
            norm = jnp.sum(jnp.transpose(square_ref[at, :]), axis=0, keepdims=True)
            if sends:
                out_ref[:rows, at] = product.astype(BF16)
            else:
                out_ref[u, :, at] = product
            if tall:
                put_norm(out_ref, rows, at, norm)
            elif u == 0:
                norm_ref[:, at] = jnp.broadcast_to(norm, (8, 256))
            else:
                norm_ref[:, at] += jnp.broadcast_to(norm, (8, 256))


def put_norm(out_ref, rows, at, norm):
    high = norm.astype(BF16).astype(F32)
    row = lax.broadcasted_iota(jnp.int32, (16, norm.shape[1]), 0)
    both = jnp.where(row == 0, high, jnp.where(row == 1, norm - high, 0.0))
    out_ref[rows : rows + 16, at] = both.astype(BF16)


VMEM = pl.BlockSpec(memory_space=pltpu.VMEM)
HBM = pl.BlockSpec(memory_space=pl.ANY)


def products(which, blocks, own, other, step, columns, first=0, sends=False, tall=False):
    n = len(which)
    rows, width = own.shape[1:]
    if sends:
        out_shape = [jax.ShapeDtypeStruct((rows + 16 if tall else rows, columns), BF16)]
    else:
        out_shape = [jax.ShapeDtypeStruct((n, rows, columns), F32)]
    if not tall:
        out_shape.append(jax.ShapeDtypeStruct((8, columns), F32))
    return pl.pallas_call(
        functools.partial(multiply, step=step, which=which, first=first, sends=sends, tall=tall),
        out_shape=out_shape,
        in_specs=[VMEM, HBM, HBM],
        out_specs=[VMEM] * len(out_shape),
        scratch_shapes=[
            pltpu.VMEM((columns, LANES), F32),
            pltpu.VMEM((columns, LANES), F32),
            pltpu.VMEM((columns, 2 * width), BF16),
            pltpu.VMEM((columns, LANES), F32),
            pltpu.VMEM((n, 2, rows, width), BF16),
            pltpu.SemaphoreType.DMA((n, 2)),
        ],
        compiler_params=pltpu.CompilerParams(vmem_limit_bytes=52 << 20),
        cost_estimate=pl.CostEstimate(
            flops=n * rows * columns * width * 4, bytes_accessed=n * 6 << 20, transcendentals=n * columns * width * 2
        ),
        name="products",
    )(blocks, own, other)


def add_on(*refs, pieces):
    got_refs, (product_ref, norm_ref), out_refs = refs[: -pieces - 2], refs[-pieces - 2 : -pieces], refs[-pieces:]
    rows = product_ref.shape[1]
    runs = max(len(got_refs), pieces)
    each = product_ref.shape[2] // runs
    for i in range(runs):
        at = slice(i * each, (i + 1) * each)
        got_ref, got_at = (got_refs[0], at) if len(got_refs) == 1 else (got_refs[i], slice(None))
        out_ref, out_at = (out_refs[0], at) if pieces == 1 else (out_refs[i], slice(None))
        out_ref[:rows, out_at] = (got_ref[:rows, got_at].astype(F32) + product_ref[0, :, at]).astype(BF16)
        if out_ref.shape[0] > rows:
            norm = jnp.sum(got_ref[rows:, got_at].astype(F32), axis=0, keepdims=True) + norm_ref[:1, at]
            put_norm(out_ref, rows, out_at, norm)


def added(got, product, norm, pieces):
    rows, columns = product.shape[1:]
    return pl.pallas_call(
        functools.partial(add_on, pieces=pieces),
        out_shape=[jax.ShapeDtypeStruct((got[0].shape[0], columns // pieces), BF16)] * pieces,
        in_specs=[VMEM] * (len(got) + 2),
        out_specs=[VMEM] * pieces,
        compiler_params=pltpu.CompilerParams(vmem_limit_bytes=8 << 20),
        cost_estimate=pl.CostEstimate(flops=rows * columns * 1000, bytes_accessed=2 << 20, transcendentals=0),
        name="add_on",
    )(*got, product, norm)


def finish(a_ref, b_ref, c_ref, d_ref, product_ref, norm_ref, out_ref, held_ref, sems):
    rows = product_ref.shape[1]
    step = rows // 2
    squares = norm_ref[:1, :]
    for ref in (a_ref, c_ref):
        squares = squares + jnp.sum(ref[rows:, :].astype(F32), axis=0, keepdims=True)
    norm = jnp.sqrt(squares)
    core = lax.axis_index("depth").astype(jnp.int32)
    stores = []
    for half, one, two in ((core, a_ref, d_ref), (1 - core, b_ref, c_ref)):
        for start in range(0, rows, step):
            at = pl.ds(start, step)
            total = product_ref[half, at] + one[at, :].astype(F32) + two[at, :].astype(F32)
            held_ref[len(stores)] = total / norm
            store = pltpu.make_async_copy(held_ref.at[len(stores)], out_ref.at[half, at], sems.at[len(stores)])
            store.start()
            stores.append(store)
    for store in stores:
        store.wait()


def finished(first, second, first_across, second_across, product, norm):
    _, rows, columns = product.shape
    return pl.pallas_call(
        finish,
        out_shape=jax.ShapeDtypeStruct(product.shape, F32),
        in_specs=[VMEM] * 6,
        out_specs=HBM,
        scratch_shapes=[pltpu.VMEM((4, rows // 2, columns), F32), pltpu.SemaphoreType.DMA((4,))],
        cost_estimate=pl.CostEstimate(flops=product.size * 100, bytes_accessed=4 << 20, transcendentals=0),
        compiler_params=pltpu.CompilerParams(vmem_limit_bytes=8 << 20),
        name="finish",
    )(first, second, first_across, second_across, product, norm)


def pack(spectrum_ref, wanted_ref, fraction_ref, out_ref, held_ref, wanted_held, fraction_held, sems):
    loads = []
    for i, (ref, held) in enumerate(((spectrum_ref, held_ref), (wanted_ref, wanted_held), (fraction_ref, fraction_held))):
        loads.append(pltpu.make_async_copy(ref, held, sems.at[i]))
    for load in loads:
        load.start()
    for load in loads:
        load.wait()
    rows = []
    for half in range(2):
        for start in range(0, held_ref.shape[1], LANES):
            rows.append(held_ref[half : half + 1, start : start + LANES])
    for ref in (wanted_held, fraction_held):
        for start in range(0, ref.shape[1], LANES):
            rows.append(ref[:, start : start + LANES].astype(F32))
    out_ref[...] = jnp.concatenate(rows, axis=0)


def packed(spectrum, wanted, fraction):
    arrays = (spectrum, wanted.reshape(1, -1), fraction.reshape(1, -1))
    rows = sum(x.size for x in arrays) // LANES
    return pl.pallas_call(
        pack,
        out_shape=jax.ShapeDtypeStruct((rows, LANES), F32),
        in_specs=[HBM] * 3,
        out_specs=VMEM,
        scratch_shapes=[pltpu.VMEM(x.shape, x.dtype) for x in arrays] + [pltpu.SemaphoreType.DMA((3,))],
        compiler_params=pltpu.CompilerParams(vmem_limit_bytes=62 << 20),
        cost_estimate=pl.CostEstimate(flops=1000, bytes_accessed=400000, transcendentals=0),
        name="pack",
    )(*arrays)


def body(halves, spectrum, wanted, fraction):
    rows = halves.shape[1]
    ncols = lax.axis_size("col")
    ndepth = lax.axis_size("depth")
    nrows = lax.axis_size(ROW)
    columns = wanted.shape[0]
    reach = ncols // 2
    ring = ("col", "depth")

    def along(core, col, by):
        return (col + (by if core == 0 else -by)) % ncols

    straight = [(k * ndepth + c, along(c, k, 1) * ndepth + c) for k in range(ncols) for c in range(ndepth)]
    across = [(k * ndepth + c, along(c, k, 1) * ndepth + 1 - c) for k in range(ncols) for c in range(ndepth)]

    other = lax.ppermute(halves, "depth", [(0, 1), (1, 0)])
    pairs = []
    for r in range(nrows):
        for k in range(ncols):
            for c in range(ndepth):
                source = along(c, k, r // 2) * ndepth + (c ^ (r & 1))
                pairs.append((r * ncols * ndepth + source, r * ncols * ndepth + k * ndepth + c))
    theirs = lax.ppermute(packed(spectrum, wanted, fraction), ROW + ring, pairs)
    last = lax.axis_index(ROW) == nrows - 1
    edge = [jnp.where(last, h[0, rows - 1], h[1, 0]).astype(F32).reshape(-1, LANES) for h in (halves, other)]
    parcel = jnp.concatenate([theirs] + edge, axis=0)
    blocks = lax.all_to_all(jnp.broadcast_to(parcel[None], (nrows,) + parcel.shape), ROW, 0, 0, tiled=True)

    multiplied = functools.partial(products, blocks=blocks, own=halves, other=other)
    a = []
    for first in range(0, columns // LANES, 2):
        (part,) = multiplied(("first",), step=reach, first=first, columns=2 * LANES, sends=True, tall=True)
        a.append(lax.ppermute(part, ring, straight))
    b, norm = multiplied(("second",), step=reach - 1, columns=columns, sends=True)
    b = lax.ppermute(b, ring, straight)
    product, more = multiplied(("first",), step=reach - 1, columns=columns)
    (a,) = added(a, product, norm + more, 1)
    for step in range(reach - 2, 0, -1):
        a = lax.ppermute(a, ring, straight)
        product, norm = multiplied(("second",), step=step, columns=columns)
        pieces = 1 if step > 1 else 2
        b, *b_across = added([b], product, norm, pieces)
        b = lax.ppermute(b, ring, straight)
        b_across = [lax.ppermute(x, ring, across) for x in b_across]
        product, more = multiplied(("first",), step=step, columns=columns)
        a, *a_across = added([a], product, norm + more, pieces)
    a = lax.ppermute(a, ring, straight)
    a_across = [lax.ppermute(x, ring, across) for x in a_across]
    product, norm = multiplied((0, 1), step=0, columns=columns // ndepth)
    return finished(a, b, a_across[0], b_across[0], product, norm)


def solution(mesh):
    split = Mesh(
        mesh.devices.reshape(4, 4, mesh.shape["col"], mesh.shape["depth"]), ("row_0", "row_1", "col", "depth")
    )
    in_specs = (P(None, ROW, ("col", "depth")), P(None, ("col", "depth")), P("col"), P("col"))
    out_specs = P(None, ROW, ("col", "depth"))
    return jax.shard_map(body, mesh=split, in_specs=in_specs, out_specs=out_specs, check_vma=False)
```

```python
import functools

import jax
import jax.numpy as jnp
from jax import lax
from jax.experimental import pallas as pl
from jax.experimental.pallas import tpu as pltpu
from jax.sharding import Mesh
from jax.sharding import PartitionSpec as P


ROW = ("row_0", "row_1")
LANES = 128
PIECE = 64
F32 = jnp.float32
BF16 = jnp.bfloat16


def look_up(core, col, blocks_ref, low_ref, shift_ref, *, step, value_rows, count):
    places = blocks_ref.shape[0]
    table = blocks_ref[:, :value_rows, :].reshape(places * value_rows, LANES)
    high = table.astype(BF16)
    rest = table - high.astype(F32)
    middle = rest.astype(BF16)
    small = (rest - middle.astype(F32)).astype(BF16)
    split = jnp.concatenate([high, middle, small], axis=1)
    per_block = value_rows * LANES
    half = per_block // 2

    roots = blocks_ref[2 * step, value_rows : value_rows + 8, :]
    swapped = jnp.concatenate([roots[2:4], roots[0:2], roots[6:8], roots[4:6]], axis=0)
    roots = jnp.where(core == 0, roots, swapped)
    wanted = roots[:4].astype(jnp.int32)
    rows = []
    for position in (wanted, wanted + 1):
        owner = lax.shift_right_logical(position, per_block.bit_length() - 1)
        ahead = lax.shift_right_logical(owner, 1) - col
        ahead = jnp.where(core == 0, ahead, -ahead) & (places // 2 - 1)
        owner = ahead * 2 + ((owner & 1) ^ core)
        inside = position & (per_block - 1)
        index = (inside & 1) * half + lax.shift_right_logical(inside, 1)
        rows += [owner * value_rows + lax.shift_right_logical(index, 7), index & (LANES - 1)]
    rows = jnp.concatenate([r.astype(F32) for r in rows] + [roots[4:], jnp.zeros((LANES - 20, LANES), F32)], axis=0)
    spots = jnp.transpose(rows)
    row_ids = lax.broadcasted_iota(jnp.int32, (LANES, places * value_rows), 1).astype(F32)
    lane_ids = lax.broadcasted_iota(jnp.int32, (LANES, LANES), 1).astype(F32)
    for tile in range(count):
        picks = [jnp.where(row_ids == spots[:, k + tile : k + tile + 1], 1.0, 0.0).astype(BF16) for k in (0, 8)]
        got = jnp.dot(jnp.concatenate(picks, axis=0), split, preferred_element_type=F32)
        got = (got[:, :LANES] + got[:, LANES : 2 * LANES]) + got[:, 2 * LANES :]
        lower, upper = (
            jnp.sum(jnp.where(lane_ids == spots[:, k + tile : k + tile + 1], got[at : at + LANES], 0.0), axis=1, keepdims=True)
            for k, at in ((4, 0), (12, LANES))
        )
        shift = spots[:, 16 + tile : 17 + tile] * (upper - lower)
        at = slice(tile * LANES, (tile + 1) * LANES)
        low_ref[at, :] = jnp.broadcast_to(lower, (LANES, LANES))
        shift_ref[at, :] = jnp.broadcast_to(shift, (LANES, LANES))


def multiply(blocks_ref, own_ref, other_ref, *refs, step, which, sends, tall, found):
    block_ref, square_ref, halves_ref, sems = refs[-4:]
    refs = refs[:-4]
    if found:
        low_ref, shift_ref, *outs = refs
    else:
        *outs, low_ref, shift_ref = refs
    out_ref, norm_ref = outs[0], None if tall else outs[1]
    columns = low_ref.shape[0]
    _, width = halves_ref.shape[2:]
    tiles = width // LANES
    value_rows = 2 * tiles
    core = lax.axis_index("depth").astype(jnp.int32)
    col = lax.axis_index("col").astype(jnp.int32)
    halves = [core if w == "first" else 1 - core if w == "second" else w for w in which]
    loads = [
        [
            pltpu.make_async_copy(ref.at[half], halves_ref.at[u, source], sems.at[u, source])
            for source, ref in enumerate((own_ref, other_ref))
        ]
        for u, half in enumerate(halves)
    ]
    for pair in loads:
        for load in pair:
            load.start()
    if not found:
        look_up(core, col, blocks_ref, low_ref, shift_ref, step=step, value_rows=value_rows, count=columns // LANES)
    for u, half in enumerate(halves):
        values = [[blocks_ref[s, pl.ds(half * tiles + t, 1), :] for t in range(tiles)] for s in range(2)]
        edge = blocks_ref[jnp.where(half == 0, blocks_ref.shape[0] - 1, 0), value_rows + 8 :, :]
        seams = [[edge[s * tiles + t : s * tiles + t + 1] for t in range(tiles)] for s in range(2)]
        for part in range(columns // 256):
            for piece in range(256 // PIECE):
                start = part * 256 + piece * PIECE
                low = low_ref[start : start + PIECE, :]
                shift = shift_ref[start : start + PIECE, :]
                square = jnp.zeros((PIECE, LANES), F32)
                for source in range(2):
                    for tile in range(tiles):
                        cauchy = seams[source][tile] / ((values[source][tile] - low) - shift)
                        square = square + cauchy * cauchy
                        begin = source * width + tile * LANES
                        block_ref[start : start + PIECE, begin : begin + LANES] = cauchy.astype(BF16)
                square_ref[start : start + PIECE, :] = square
            if part == WAIT_AT[found] or part == columns // 256 - 1 and columns // 256 <= WAIT_AT[found]:
                for load in loads[u]:
                    load.wait()
                for done in range(part):
                    multiply_out(u, done, out_ref, norm_ref, block_ref, square_ref, halves_ref, sends, tall)
            if part >= WAIT_AT[found] or columns // 256 <= WAIT_AT[found]:
                multiply_out(u, part, out_ref, norm_ref, block_ref, square_ref, halves_ref, sends, tall)


WAIT_AT = {False: 0, True: 1}


def multiply_out(u, part, out_ref, norm_ref, block_ref, square_ref, halves_ref, sends, tall):
    nt = (((1,), (1,)), ((), ()))
    rows, width = halves_ref.shape[2:]
    at = slice(part * 256, (part + 1) * 256)
    product = lax.dot_general(halves_ref[u, 0], block_ref[at, :width], nt, preferred_element_type=F32)
    product = product + lax.dot_general(halves_ref[u, 1], block_ref[at, width:], nt, preferred_element_type=F32)
    norm = jnp.sum(jnp.transpose(square_ref[at, :]), axis=0, keepdims=True)
    if sends:
        out_ref[:rows, at] = product.astype(BF16)
    else:
        out_ref[u, :, at] = product
    if tall:
        put_norm(out_ref, rows, at, norm)
    elif u == 0:
        norm_ref[:, at] = jnp.broadcast_to(norm, (8, 256))
    else:
        norm_ref[:, at] += jnp.broadcast_to(norm, (8, 256))


def put_norm(out_ref, rows, at, norm):
    high = norm.astype(BF16).astype(F32)
    row = lax.broadcasted_iota(jnp.int32, (16, norm.shape[1]), 0)
    both = jnp.where(row == 0, high, jnp.where(row == 1, norm - high, 0.0))
    out_ref[rows : rows + 16, at] = both.astype(BF16)


VMEM = pl.BlockSpec(memory_space=pltpu.VMEM)
HBM = pl.BlockSpec(memory_space=pl.ANY)


def products(which, blocks, own, other, step, columns, sends=False, tall=False, found=()):
    n = len(which)
    rows, width = own.shape[1:]
    if sends:
        out_shape = [jax.ShapeDtypeStruct((rows + 16 if tall else rows, columns), BF16)]
    else:
        out_shape = [jax.ShapeDtypeStruct((n, rows, columns), F32)]
    if not tall:
        out_shape.append(jax.ShapeDtypeStruct((8, columns), F32))
    scratch = [
        pltpu.VMEM((columns, 2 * width), BF16),
        pltpu.VMEM((columns, LANES), F32),
        pltpu.VMEM((n, 2, rows, width), BF16),
        pltpu.SemaphoreType.DMA((n, 2)),
    ]
    keeps = not found and not tall and n == 1
    if keeps:
        out_shape += [jax.ShapeDtypeStruct((columns, LANES), F32)] * 2
    elif not found:
        scratch = [pltpu.VMEM((columns, LANES), F32)] * 2 + scratch
    return pl.pallas_call(
        functools.partial(multiply, step=step, which=which, sends=sends, tall=tall, found=bool(found)),
        out_shape=out_shape,
        in_specs=[VMEM, HBM, HBM] + [VMEM] * len(found),
        out_specs=[VMEM] * len(out_shape),
        scratch_shapes=scratch,
        compiler_params=pltpu.CompilerParams(vmem_limit_bytes=52 << 20),
        cost_estimate=pl.CostEstimate(
            flops=n * rows * columns * width * 4, bytes_accessed=n * 6 << 20, transcendentals=n * columns * width * 2
        ),
        name="products",
    )(blocks, own, other, *found)


def add_on(*refs, pieces):
    got_refs, (product_ref, norm_ref), out_refs = refs[: -pieces - 2], refs[-pieces - 2 : -pieces], refs[-pieces:]
    rows = product_ref.shape[1]
    runs = max(len(got_refs), pieces)
    each = product_ref.shape[2] // runs
    for i in range(runs):
        at = slice(i * each, (i + 1) * each)
        got_ref, got_at = (got_refs[0], at) if len(got_refs) == 1 else (got_refs[i], slice(None))
        out_ref, out_at = (out_refs[0], at) if pieces == 1 else (out_refs[i], slice(None))
        out_ref[:rows, out_at] = (got_ref[:rows, got_at].astype(F32) + product_ref[0, :, at]).astype(BF16)
        if out_ref.shape[0] > rows:
            norm = jnp.sum(got_ref[rows:, got_at].astype(F32), axis=0, keepdims=True) + norm_ref[:1, at]
            put_norm(out_ref, rows, out_at, norm)


def added(got, product, norm, pieces):
    rows, columns = product.shape[1:]
    return pl.pallas_call(
        functools.partial(add_on, pieces=pieces),
        out_shape=[jax.ShapeDtypeStruct((got[0].shape[0], columns // pieces), BF16)] * pieces,
        in_specs=[VMEM] * (len(got) + 2),
        out_specs=[VMEM] * pieces,
        compiler_params=pltpu.CompilerParams(vmem_limit_bytes=8 << 20),
        cost_estimate=pl.CostEstimate(flops=rows * columns * 1000, bytes_accessed=2 << 20, transcendentals=0),
        name="add_on",
    )(*got, product, norm)


def finish(a_ref, b_ref, c_ref, d_ref, product_ref, norm_ref, out_ref, held_ref, sems):
    rows = product_ref.shape[1]
    step = rows // 2
    squares = norm_ref[:1, :]
    for ref in (a_ref, c_ref):
        squares = squares + jnp.sum(ref[rows:, :].astype(F32), axis=0, keepdims=True)
    norm = jnp.sqrt(squares)
    core = lax.axis_index("depth").astype(jnp.int32)
    stores = []
    for half, one, two in ((core, a_ref, d_ref), (1 - core, b_ref, c_ref)):
        for start in range(0, rows, step):
            at = pl.ds(start, step)
            total = product_ref[half, at] + one[at, :].astype(F32) + two[at, :].astype(F32)
            held_ref[len(stores)] = total / norm
            store = pltpu.make_async_copy(held_ref.at[len(stores)], out_ref.at[half, at], sems.at[len(stores)])
            store.start()
            stores.append(store)
    for store in stores:
        store.wait()


def finished(first, second, first_across, second_across, product, norm):
    _, rows, columns = product.shape
    return pl.pallas_call(
        finish,
        out_shape=jax.ShapeDtypeStruct(product.shape, F32),
        in_specs=[VMEM] * 6,
        out_specs=HBM,
        scratch_shapes=[pltpu.VMEM((4, rows // 2, columns), F32), pltpu.SemaphoreType.DMA((4,))],
        cost_estimate=pl.CostEstimate(flops=product.size * 100, bytes_accessed=4 << 20, transcendentals=0),
        compiler_params=pltpu.CompilerParams(vmem_limit_bytes=8 << 20),
        name="finish",
    )(first, second, first_across, second_across, product, norm)


def pack(spectrum_ref, wanted_ref, fraction_ref, out_ref, held_ref, wanted_held, fraction_held, sems):
    loads = []
    for i, (ref, held) in enumerate(((spectrum_ref, held_ref), (wanted_ref, wanted_held), (fraction_ref, fraction_held))):
        loads.append(pltpu.make_async_copy(ref, held, sems.at[i]))
    for load in loads:
        load.start()
    for load in loads:
        load.wait()
    rows = []
    for half in range(2):
        for start in range(0, held_ref.shape[1], LANES):
            rows.append(held_ref[half : half + 1, start : start + LANES])
    for ref in (wanted_held, fraction_held):
        for start in range(0, ref.shape[1], LANES):
            rows.append(ref[:, start : start + LANES].astype(F32))
    out_ref[...] = jnp.concatenate(rows, axis=0)


def packed(spectrum, wanted, fraction):
    arrays = (spectrum, wanted.reshape(1, -1), fraction.reshape(1, -1))
    rows = sum(x.size for x in arrays) // LANES
    return pl.pallas_call(
        pack,
        out_shape=jax.ShapeDtypeStruct((rows, LANES), F32),
        in_specs=[HBM] * 3,
        out_specs=VMEM,
        scratch_shapes=[pltpu.VMEM(x.shape, x.dtype) for x in arrays] + [pltpu.SemaphoreType.DMA((3,))],
        compiler_params=pltpu.CompilerParams(vmem_limit_bytes=62 << 20),
        cost_estimate=pl.CostEstimate(flops=1000, bytes_accessed=400000, transcendentals=0),
        name="pack",
    )(*arrays)


def body(halves, spectrum, wanted, fraction):
    rows = halves.shape[1]
    ncols = lax.axis_size("col")
    ndepth = lax.axis_size("depth")
    nrows = lax.axis_size(ROW)
    columns = wanted.shape[0]
    reach = ncols // 2
    ring = ("col", "depth")

    def along(core, col, by):
        return (col + (by if core == 0 else -by)) % ncols

    straight = [(k * ndepth + c, along(c, k, 1) * ndepth + c) for k in range(ncols) for c in range(ndepth)]
    across = [(k * ndepth + c, along(c, k, 1) * ndepth + 1 - c) for k in range(ncols) for c in range(ndepth)]

    other = lax.ppermute(halves, "depth", [(0, 1), (1, 0)])
    pairs = []
    for r in range(nrows):
        for k in range(ncols):
            for c in range(ndepth):
                source = along(c, k, r // 2) * ndepth + (c ^ (r & 1))
                pairs.append((r * ncols * ndepth + source, r * ncols * ndepth + k * ndepth + c))
    theirs = lax.ppermute(packed(spectrum, wanted, fraction), ROW + ring, pairs)
    last = lax.axis_index(ROW) == nrows - 1
    edge = [jnp.where(last, h[0, rows - 1], h[1, 0]).astype(F32).reshape(-1, LANES) for h in (halves, other)]
    parcel = jnp.concatenate([theirs] + edge, axis=0)
    blocks = lax.all_to_all(jnp.broadcast_to(parcel[None], (nrows,) + parcel.shape), ROW, 0, 0, tiled=True)

    multiplied = functools.partial(products, blocks=blocks, own=halves, other=other, columns=columns)
    (a,) = multiplied(("first",), step=reach, sends=True, tall=True)
    a = lax.ppermute(a, ring, straight)
    b, norm, *found = multiplied(("second",), step=reach - 1, sends=True)
    b = lax.ppermute(b, ring, straight)
    product, more = multiplied(("first",), step=reach - 1, found=found)
    (a,) = added([a], product, norm + more, 1)
    for step in range(reach - 2, 0, -1):
        a = lax.ppermute(a, ring, straight)
        product, norm, *found = multiplied(("second",), step=step)
        pieces = 1 if step > 1 else 2
        b, *b_across = added([b], product, norm, pieces)
        b = lax.ppermute(b, ring, straight)
        b_across = [lax.ppermute(x, ring, across) for x in b_across]
        product, more = multiplied(("first",), step=step, found=found)
        a, *a_across = added([a], product, norm + more, pieces)
    a = lax.ppermute(a, ring, straight)
    a_across = [lax.ppermute(x, ring, across) for x in a_across]
    product, norm = multiplied((0, 1), step=0, columns=columns // ndepth)
    return finished(a, b, a_across[0], b_across[0], product, norm)


def solution(mesh):
    split = Mesh(
        mesh.devices.reshape(4, 4, mesh.shape["col"], mesh.shape["depth"]), ("row_0", "row_1", "col", "depth")
    )
    in_specs = (P(None, ROW, ("col", "depth")), P(None, ("col", "depth")), P("col"), P("col"))
    out_specs = P(None, ROW, ("col", "depth"))
    return jax.shard_map(body, mesh=split, in_specs=in_specs, out_specs=out_specs, check_vma=False)
```

```python
import functools

import jax
import jax.numpy as jnp
from jax import lax
from jax.experimental import pallas as pl
from jax.experimental.pallas import tpu as pltpu
from jax.sharding import Mesh
from jax.sharding import PartitionSpec as P


ROW = ("row_0", "row_1")
LANES = 128
PIECE = 64
F32 = jnp.float32
BF16 = jnp.bfloat16


def look_up(core, col, blocks_ref, low_ref, shift_ref, *, step, value_rows, count):
    places = blocks_ref.shape[0]
    table = blocks_ref[:, :value_rows, :].reshape(places * value_rows, LANES)
    high = table.astype(BF16)
    rest = table - high.astype(F32)
    middle = rest.astype(BF16)
    small = (rest - middle.astype(F32)).astype(BF16)
    split = jnp.concatenate([high, middle, small], axis=1)
    per_block = value_rows * LANES
    half = per_block // 2

    roots = blocks_ref[2 * step, value_rows : value_rows + 8, :]
    swapped = jnp.concatenate([roots[2:4], roots[0:2], roots[6:8], roots[4:6]], axis=0)
    roots = jnp.where(core == 0, roots, swapped)
    wanted = roots[:4].astype(jnp.int32)
    rows = []
    for position in (wanted, wanted + 1):
        owner = lax.shift_right_logical(position, per_block.bit_length() - 1)
        ahead = lax.shift_right_logical(owner, 1) - col
        ahead = jnp.where(core == 0, ahead, -ahead) & (places // 2 - 1)
        owner = ahead * 2 + ((owner & 1) ^ core)
        inside = position & (per_block - 1)
        index = (inside & 1) * half + lax.shift_right_logical(inside, 1)
        rows += [owner * value_rows + lax.shift_right_logical(index, 7), index & (LANES - 1)]
    rows = jnp.concatenate([r.astype(F32) for r in rows] + [roots[4:], jnp.zeros((LANES - 20, LANES), F32)], axis=0)
    spots = jnp.transpose(rows)
    row_ids = lax.broadcasted_iota(jnp.int32, (LANES, places * value_rows), 1).astype(F32)
    lane_ids = lax.broadcasted_iota(jnp.int32, (LANES, LANES), 1).astype(F32)
    for tile in range(count):
        picks = [jnp.where(row_ids == spots[:, k + tile : k + tile + 1], 1.0, 0.0).astype(BF16) for k in (0, 8)]
        got = jnp.dot(jnp.concatenate(picks, axis=0), split, preferred_element_type=F32)
        got = (got[:, :LANES] + got[:, LANES : 2 * LANES]) + got[:, 2 * LANES :]
        lower, upper = (
            jnp.sum(jnp.where(lane_ids == spots[:, k + tile : k + tile + 1], got[at : at + LANES], 0.0), axis=1, keepdims=True)
            for k, at in ((4, 0), (12, LANES))
        )
        shift = spots[:, 16 + tile : 17 + tile] * (upper - lower)
        at = slice(tile * LANES, (tile + 1) * LANES)
        low_ref[at, :] = jnp.broadcast_to(lower, (LANES, LANES))
        shift_ref[at, :] = jnp.broadcast_to(shift, (LANES, LANES))


def multiply(blocks_ref, own_ref, other_ref, *refs, step, which, sends, tall, found):
    block_ref, square_ref, halves_ref, sems = refs[-4:]
    refs = refs[:-4]
    if found:
        low_ref, shift_ref, *outs = refs
    else:
        *outs, low_ref, shift_ref = refs
    out_ref, norm_ref = outs[0], None if tall else outs[1]
    columns = low_ref.shape[0]
    _, width = halves_ref.shape[2:]
    tiles = width // LANES
    value_rows = 2 * tiles
    core = lax.axis_index("depth").astype(jnp.int32)
    col = lax.axis_index("col").astype(jnp.int32)
    halves = [core if w == "first" else 1 - core if w == "second" else w for w in which]
    loads = [
        [
            pltpu.make_async_copy(ref.at[half], halves_ref.at[u, source], sems.at[u, source])
            for source, ref in enumerate((own_ref, other_ref))
        ]
        for u, half in enumerate(halves)
    ]
    for pair in loads:
        for load in pair:
            load.start()
    if not found:
        look_up(core, col, blocks_ref, low_ref, shift_ref, step=step, value_rows=value_rows, count=columns // LANES)
    for u, half in enumerate(halves):
        values = [[blocks_ref[s, pl.ds(half * tiles + t, 1), :] for t in range(tiles)] for s in range(2)]
        edge = blocks_ref[jnp.where(half == 0, blocks_ref.shape[0] - 1, 0), value_rows + 8 :, :]
        seams = [[edge[s * tiles + t : s * tiles + t + 1] for t in range(tiles)] for s in range(2)]
        for part in range(columns // 256):
            for piece in range(256 // PIECE):
                start = part * 256 + piece * PIECE
                low = low_ref[start : start + PIECE, :]
                shift = shift_ref[start : start + PIECE, :]
                square = jnp.zeros((PIECE, LANES), F32)
                for source in range(2):
                    for tile in range(tiles):
                        cauchy = seams[source][tile] / ((values[source][tile] - low) - shift)
                        square = square + cauchy * cauchy
                        begin = source * width + tile * LANES
                        block_ref[start : start + PIECE, begin : begin + LANES] = cauchy.astype(BF16)
                square_ref[start : start + PIECE, :] = square
            if part == WAIT_AT[found] or part == columns // 256 - 1 and columns // 256 <= WAIT_AT[found]:
                for load in loads[u]:
                    load.wait()
                for done in range(part):
                    multiply_out(u, done, out_ref, norm_ref, block_ref, square_ref, halves_ref, sends, tall)
            if part >= WAIT_AT[found] or columns // 256 <= WAIT_AT[found]:
                multiply_out(u, part, out_ref, norm_ref, block_ref, square_ref, halves_ref, sends, tall)


WAIT_AT = {False: 0, True: 1}


def multiply_out(u, part, out_ref, norm_ref, block_ref, square_ref, halves_ref, sends, tall):
    nt = (((1,), (1,)), ((), ()))
    rows, width = halves_ref.shape[2:]
    at = slice(part * 256, (part + 1) * 256)
    product = lax.dot_general(halves_ref[u, 0], block_ref[at, :width], nt, preferred_element_type=F32)
    product = product + lax.dot_general(halves_ref[u, 1], block_ref[at, width:], nt, preferred_element_type=F32)
    norm = jnp.sum(jnp.transpose(square_ref[at, :]), axis=0, keepdims=True)
    if sends:
        out_ref[:rows, at] = product.astype(BF16)
    else:
        out_ref[u, :, at] = product
    if tall:
        put_norm(out_ref, rows, at, norm)
    elif u == 0:
        norm_ref[:, at] = jnp.broadcast_to(norm, (8, 256))
    else:
        norm_ref[:, at] += jnp.broadcast_to(norm, (8, 256))


def put_norm(out_ref, rows, at, norm):
    high = norm.astype(BF16).astype(F32)
    row = lax.broadcasted_iota(jnp.int32, (16, norm.shape[1]), 0)
    both = jnp.where(row == 0, high, jnp.where(row == 1, norm - high, 0.0))
    out_ref[rows : rows + 16, at] = both.astype(BF16)


VMEM = pl.BlockSpec(memory_space=pltpu.VMEM)
HBM = pl.BlockSpec(memory_space=pl.ANY)


def products(which, blocks, own, other, step, columns, sends=False, tall=False, found=()):
    n = len(which)
    rows, width = own.shape[1:]
    if sends:
        out_shape = [jax.ShapeDtypeStruct((rows + 16 if tall else rows, columns), BF16)]
    else:
        out_shape = [jax.ShapeDtypeStruct((n, rows, columns), F32)]
    if not tall:
        out_shape.append(jax.ShapeDtypeStruct((8, columns), F32))
    scratch = [
        pltpu.VMEM((columns, 2 * width), BF16),
        pltpu.VMEM((columns, LANES), F32),
        pltpu.VMEM((n, 2, rows, width), BF16),
        pltpu.SemaphoreType.DMA((n, 2)),
    ]
    keeps = not found and not tall and n == 1
    if keeps:
        out_shape += [jax.ShapeDtypeStruct((columns, LANES), F32)] * 2
    elif not found:
        scratch = [pltpu.VMEM((columns, LANES), F32)] * 2 + scratch
    return pl.pallas_call(
        functools.partial(multiply, step=step, which=which, sends=sends, tall=tall, found=bool(found)),
        out_shape=out_shape,
        in_specs=[VMEM, HBM, HBM] + [VMEM] * len(found),
        out_specs=[VMEM] * len(out_shape),
        scratch_shapes=scratch,
        compiler_params=pltpu.CompilerParams(vmem_limit_bytes=52 << 20),
        cost_estimate=pl.CostEstimate(
            flops=n * rows * columns * width * 4, bytes_accessed=n * 6 << 20, transcendentals=n * columns * width * 2
        ),
        name="products",
    )(blocks, own, other, *found)


def add_on(*refs, pieces):
    got_refs, (product_ref, norm_ref), out_refs = refs[: -pieces - 2], refs[-pieces - 2 : -pieces], refs[-pieces:]
    rows = product_ref.shape[1]
    runs = max(len(got_refs), pieces)
    each = product_ref.shape[2] // runs
    for i in range(runs):
        at = slice(i * each, (i + 1) * each)
        got_ref, got_at = (got_refs[0], at) if len(got_refs) == 1 else (got_refs[i], slice(None))
        out_ref, out_at = (out_refs[0], at) if pieces == 1 else (out_refs[i], slice(None))
        out_ref[:rows, out_at] = (got_ref[:rows, got_at].astype(F32) + product_ref[0, :, at]).astype(BF16)
        if out_ref.shape[0] > rows:
            norm = jnp.sum(got_ref[rows:, got_at].astype(F32), axis=0, keepdims=True) + norm_ref[:1, at]
            put_norm(out_ref, rows, out_at, norm)


def added(got, product, norm, pieces):
    rows, columns = product.shape[1:]
    return pl.pallas_call(
        functools.partial(add_on, pieces=pieces),
        out_shape=[jax.ShapeDtypeStruct((got[0].shape[0], columns // pieces), BF16)] * pieces,
        in_specs=[VMEM] * (len(got) + 2),
        out_specs=[VMEM] * pieces,
        compiler_params=pltpu.CompilerParams(vmem_limit_bytes=8 << 20),
        cost_estimate=pl.CostEstimate(flops=rows * columns * 1000, bytes_accessed=2 << 20, transcendentals=0),
        name="add_on",
    )(*got, product, norm)


def finish(a_ref, b_ref, c_ref, d_ref, product_ref, norm_ref, out_ref, held_ref, sems):
    rows = product_ref.shape[1]
    step = rows // 2
    squares = norm_ref[:1, :]
    for ref in (a_ref, c_ref):
        squares = squares + jnp.sum(ref[rows:, :].astype(F32), axis=0, keepdims=True)
    norm = jnp.sqrt(squares)
    core = lax.axis_index("depth").astype(jnp.int32)
    stores = []
    for half, one, two in ((core, a_ref, d_ref), (1 - core, b_ref, c_ref)):
        for start in range(0, rows, step):
            at = pl.ds(start, step)
            total = product_ref[half, at] + one[at, :].astype(F32) + two[at, :].astype(F32)
            held_ref[len(stores)] = total / norm
            store = pltpu.make_async_copy(held_ref.at[len(stores)], out_ref.at[half, at], sems.at[len(stores)])
            store.start()
            stores.append(store)
    for store in stores:
        store.wait()


def finished(first, second, first_across, second_across, product, norm):
    _, rows, columns = product.shape
    return pl.pallas_call(
        finish,
        out_shape=jax.ShapeDtypeStruct(product.shape, F32),
        in_specs=[VMEM] * 6,
        out_specs=HBM,
        scratch_shapes=[pltpu.VMEM((4, rows // 2, columns), F32), pltpu.SemaphoreType.DMA((4,))],
        cost_estimate=pl.CostEstimate(flops=product.size * 100, bytes_accessed=4 << 20, transcendentals=0),
        compiler_params=pltpu.CompilerParams(vmem_limit_bytes=8 << 20),
        name="finish",
    )(first, second, first_across, second_across, product, norm)


def pack(spectrum_ref, wanted_ref, fraction_ref, out_ref, held_ref, wanted_held, fraction_held, sems):
    loads = []
    for i, (ref, held) in enumerate(((spectrum_ref, held_ref), (wanted_ref, wanted_held), (fraction_ref, fraction_held))):
        loads.append(pltpu.make_async_copy(ref, held, sems.at[i]))
    for load in loads:
        load.start()
    for load in loads:
        load.wait()
    rows = []
    for half in range(2):
        for start in range(0, held_ref.shape[1], LANES):
            rows.append(held_ref[half : half + 1, start : start + LANES])
    for ref in (wanted_held, fraction_held):
        for start in range(0, ref.shape[1], LANES):
            rows.append(ref[:, start : start + LANES].astype(F32))
    out_ref[...] = jnp.concatenate(rows, axis=0)


def packed(spectrum, wanted, fraction):
    arrays = (spectrum, wanted.reshape(1, -1), fraction.reshape(1, -1))
    rows = sum(x.size for x in arrays) // LANES
    return pl.pallas_call(
        pack,
        out_shape=jax.ShapeDtypeStruct((rows, LANES), F32),
        in_specs=[HBM] * 3,
        out_specs=VMEM,
        scratch_shapes=[pltpu.VMEM(x.shape, x.dtype) for x in arrays] + [pltpu.SemaphoreType.DMA((3,))],
        compiler_params=pltpu.CompilerParams(vmem_limit_bytes=62 << 20),
        cost_estimate=pl.CostEstimate(flops=1000, bytes_accessed=400000, transcendentals=0),
        name="pack",
    )(*arrays)


def body(halves, spectrum, wanted, fraction):
    rows = halves.shape[1]
    ncols = lax.axis_size("col")
    ndepth = lax.axis_size("depth")
    nrows = lax.axis_size(ROW)
    columns = wanted.shape[0]
    reach = ncols // 2
    ring = ("col", "depth")

    def along(core, col, by):
        return (col + (by if core == 0 else -by)) % ncols

    straight = [(k * ndepth + c, along(c, k, 1) * ndepth + c) for k in range(ncols) for c in range(ndepth)]
    across = [(k * ndepth + c, along(c, k, 1) * ndepth + 1 - c) for k in range(ncols) for c in range(ndepth)]

    other = lax.ppermute(halves, "depth", [(0, 1), (1, 0)])
    pairs = []
    for r in range(nrows):
        for k in range(ncols):
            for c in range(ndepth):
                source = along(c, k, (r or nrows - 1) // 2) * ndepth + (c ^ ((r or nrows - 1) & 1))
                pairs.append((r * ncols * ndepth + source, r * ncols * ndepth + k * ndepth + c))
    mine = packed(spectrum, wanted, fraction)
    theirs = lax.ppermute(mine, ROW + ring, pairs)
    theirs = jnp.where(lax.axis_index(ROW) == 0, mine, theirs)
    last = lax.axis_index(ROW) == nrows - 1
    edge = [jnp.where(last, h[0, rows - 1], h[1, 0]).astype(F32).reshape(-1, LANES) for h in (halves, other)]
    parcel = jnp.concatenate([theirs] + edge, axis=0)
    blocks = lax.all_to_all(jnp.broadcast_to(parcel[None], (nrows,) + parcel.shape), ROW, 0, 0, tiled=True)

    multiplied = functools.partial(products, blocks=blocks, own=halves, other=other, columns=columns)
    (a,) = multiplied(("first",), step=reach, sends=True, tall=True)
    a = lax.ppermute(a, ring, straight)
    b, norm, *found = multiplied(("second",), step=reach - 1, sends=True)
    b = lax.ppermute(b, ring, straight)
    product, more = multiplied(("first",), step=reach - 1, found=found)
    (a,) = added([a], product, norm + more, 1)
    for step in range(reach - 2, 0, -1):
        a = lax.ppermute(a, ring, straight)
        product, norm, *found = multiplied(("second",), step=step)
        pieces = 1 if step > 1 else 2
        b, *b_across = added([b], product, norm, pieces)
        b = lax.ppermute(b, ring, straight)
        b_across = [lax.ppermute(x, ring, across) for x in b_across]
        product, more = multiplied(("first",), step=step, found=found)
        a, *a_across = added([a], product, norm + more, pieces)
    a = lax.ppermute(a, ring, straight)
    a_across = [lax.ppermute(x, ring, across) for x in a_across]
    product, norm = multiplied((0, 1), step=0, columns=columns // ndepth)
    return finished(a, b, a_across[0], b_across[0], product, norm)


def solution(mesh):
    split = Mesh(
        mesh.devices.reshape(4, 4, mesh.shape["col"], mesh.shape["depth"]), ("row_0", "row_1", "col", "depth")
    )
    in_specs = (P(None, ROW, ("col", "depth")), P(None, ("col", "depth")), P("col"), P("col"))
    out_specs = P(None, ROW, ("col", "depth"))
    return jax.shard_map(body, mesh=split, in_specs=in_specs, out_specs=out_specs, check_vma=False)
```

```python
import functools

import jax
import jax.numpy as jnp
from jax import lax
from jax.experimental import pallas as pl
from jax.experimental.pallas import tpu as pltpu
from jax.sharding import Mesh
from jax.sharding import PartitionSpec as P


ROW = ("row_0", "row_1")
LANES = 128
PIECE = 64
F32 = jnp.float32
BF16 = jnp.bfloat16


def look_up(core, col, blocks_ref, low_ref, shift_ref, *, step, value_rows, count):
    places = blocks_ref.shape[0]
    table = blocks_ref[:, :value_rows, :].reshape(places * value_rows, LANES) * 0.25
    high = table.astype(BF16)
    rest = table - high.astype(F32)
    middle = rest.astype(BF16)
    small = (rest - middle.astype(F32)).astype(BF16)
    split = jnp.concatenate([high, middle, small], axis=1)
    per_block = value_rows * LANES
    half = per_block // 2

    roots = blocks_ref[2 * step, value_rows : value_rows + 8, :]
    swapped = jnp.concatenate([roots[2:4], roots[0:2], roots[6:8], roots[4:6]], axis=0)
    roots = jnp.where(core == 0, roots, swapped)
    wanted = roots[:4].astype(jnp.int32)
    rows = []
    for position in (wanted, wanted + 1):
        owner = lax.shift_right_logical(position, per_block.bit_length() - 1)
        ahead = lax.shift_right_logical(owner, 1) - col
        ahead = jnp.where(core == 0, ahead, -ahead) & (places // 2 - 1)
        owner = ahead * 2 + ((owner & 1) ^ core)
        inside = position & (per_block - 1)
        index = (inside & 1) * half + lax.shift_right_logical(inside, 1)
        rows += [owner * value_rows + lax.shift_right_logical(index, 7), index & (LANES - 1)]
    rows = jnp.concatenate([r.astype(F32) for r in rows] + [roots[4:], jnp.zeros((LANES - 20, LANES), F32)], axis=0)
    spots = jnp.transpose(rows)
    row_ids = lax.broadcasted_iota(jnp.int32, (LANES, places * value_rows), 1).astype(F32)
    lane_ids = lax.broadcasted_iota(jnp.int32, (LANES, LANES), 1).astype(F32)
    for tile in range(count):
        picks = [jnp.where(row_ids == spots[:, k + tile : k + tile + 1], 1.0, 0.0).astype(BF16) for k in (0, 8)]
        got = jnp.dot(jnp.concatenate(picks, axis=0), split, preferred_element_type=F32)
        got = ((got[:, :LANES] + got[:, LANES : 2 * LANES]) + got[:, 2 * LANES :]) * 4.0
        lower, upper = (
            jnp.sum(jnp.where(lane_ids == spots[:, k + tile : k + tile + 1], got[at : at + LANES], 0.0), axis=1, keepdims=True)
            for k, at in ((4, 0), (12, LANES))
        )
        shift = spots[:, 16 + tile : 17 + tile] * (upper - lower)
        at = slice(tile * LANES, (tile + 1) * LANES)
        low_ref[at, :] = jnp.broadcast_to(lower, (LANES, LANES))
        shift_ref[at, :] = jnp.broadcast_to(shift, (LANES, LANES))


def multiply(blocks_ref, own_ref, other_ref, *refs, step, which, sends, tall, found):
    block_ref, square_ref, halves_ref, sems = refs[-4:]
    refs = refs[:-4]
    if found:
        low_ref, shift_ref, *outs = refs
    else:
        *outs, low_ref, shift_ref = refs
    out_ref, norm_ref = outs[0], None if tall else outs[1]
    columns = low_ref.shape[0]
    _, width = halves_ref.shape[2:]
    tiles = width // LANES
    value_rows = 2 * tiles
    core = lax.axis_index("depth").astype(jnp.int32)
    col = lax.axis_index("col").astype(jnp.int32)
    halves = [core if w == "first" else 1 - core if w == "second" else w for w in which]
    loads = [
        [
            pltpu.make_async_copy(ref.at[half], halves_ref.at[u, source], sems.at[u, source])
            for source, ref in enumerate((own_ref, other_ref))
        ]
        for u, half in enumerate(halves)
    ]
    for pair in loads:
        for load in pair:
            load.start()
    if not found:
        look_up(core, col, blocks_ref, low_ref, shift_ref, step=step, value_rows=value_rows, count=columns // LANES)
    for u, half in enumerate(halves):
        values = [[blocks_ref[s, pl.ds(half * tiles + t, 1), :] for t in range(tiles)] for s in range(2)]
        edge = blocks_ref[jnp.where(half == 0, blocks_ref.shape[0] - 1, 0), value_rows + 8 :, :]
        seams = [[edge[s * tiles + t : s * tiles + t + 1] for t in range(tiles)] for s in range(2)]
        for part in range(columns // 256):
            for piece in range(256 // PIECE):
                start = part * 256 + piece * PIECE
                low = low_ref[start : start + PIECE, :]
                shift = shift_ref[start : start + PIECE, :]
                square = jnp.zeros((PIECE, LANES), F32)
                for source in range(2):
                    for tile in range(tiles):
                        cauchy = seams[source][tile] / ((values[source][tile] - low) - shift)
                        square = square + cauchy * cauchy
                        begin = source * width + tile * LANES
                        block_ref[start : start + PIECE, begin : begin + LANES] = cauchy.astype(BF16)
                square_ref[start : start + PIECE, :] = square
            if part == WAIT_AT[found] or part == columns // 256 - 1 and columns // 256 <= WAIT_AT[found]:
                for load in loads[u]:
                    load.wait()
                for done in range(part):
                    multiply_out(u, done, out_ref, norm_ref, block_ref, square_ref, halves_ref, sends, tall)
            if part >= WAIT_AT[found] or columns // 256 <= WAIT_AT[found]:
                multiply_out(u, part, out_ref, norm_ref, block_ref, square_ref, halves_ref, sends, tall)


WAIT_AT = {False: 0, True: 1}


def multiply_out(u, part, out_ref, norm_ref, block_ref, square_ref, halves_ref, sends, tall):
    nt = (((1,), (1,)), ((), ()))
    rows, width = halves_ref.shape[2:]
    at = slice(part * 256, (part + 1) * 256)
    product = lax.dot_general(halves_ref[u, 0], block_ref[at, :width], nt, preferred_element_type=F32)
    product = product + lax.dot_general(halves_ref[u, 1], block_ref[at, width:], nt, preferred_element_type=F32)
    norm = jnp.sum(jnp.transpose(square_ref[at, :]), axis=0, keepdims=True)
    if sends:
        out_ref[:rows, at] = product.astype(BF16)
    else:
        out_ref[u, :, at] = product
    if tall:
        put_norm(out_ref, rows, at, norm)
    elif u == 0:
        norm_ref[:, at] = jnp.broadcast_to(norm, (8, 256))
    else:
        norm_ref[:, at] += jnp.broadcast_to(norm, (8, 256))


def put_norm(out_ref, rows, at, norm):
    high = norm.astype(BF16).astype(F32)
    row = lax.broadcasted_iota(jnp.int32, (16, norm.shape[1]), 0)
    both = jnp.where(row == 0, high, jnp.where(row == 1, norm - high, 0.0))
    out_ref[rows : rows + 16, at] = both.astype(BF16)


VMEM = pl.BlockSpec(memory_space=pltpu.VMEM)
HBM = pl.BlockSpec(memory_space=pl.ANY)


def products(which, blocks, own, other, step, columns, sends=False, tall=False, found=()):
    n = len(which)
    rows, width = own.shape[1:]
    if sends:
        out_shape = [jax.ShapeDtypeStruct((rows + 16 if tall else rows, columns), BF16)]
    else:
        out_shape = [jax.ShapeDtypeStruct((n, rows, columns), F32)]
    if not tall:
        out_shape.append(jax.ShapeDtypeStruct((8, columns), F32))
    scratch = [
        pltpu.VMEM((columns, 2 * width), BF16),
        pltpu.VMEM((columns, LANES), F32),
        pltpu.VMEM((n, 2, rows, width), BF16),
        pltpu.SemaphoreType.DMA((n, 2)),
    ]
    keeps = not found and not tall and n == 1
    if keeps:
        out_shape += [jax.ShapeDtypeStruct((columns, LANES), F32)] * 2
    elif not found:
        scratch = [pltpu.VMEM((columns, LANES), F32)] * 2 + scratch
    return pl.pallas_call(
        functools.partial(multiply, step=step, which=which, sends=sends, tall=tall, found=bool(found)),
        out_shape=out_shape,
        in_specs=[VMEM, HBM, HBM] + [VMEM] * len(found),
        out_specs=[VMEM] * len(out_shape),
        scratch_shapes=scratch,
        compiler_params=pltpu.CompilerParams(vmem_limit_bytes=52 << 20),
        cost_estimate=pl.CostEstimate(
            flops=n * rows * columns * width * 4, bytes_accessed=n * 6 << 20, transcendentals=n * columns * width * 2
        ),
        name="products",
    )(blocks, own, other, *found)


def add_on(*refs, pieces):
    got_refs, (product_ref, norm_ref), out_refs = refs[: -pieces - 2], refs[-pieces - 2 : -pieces], refs[-pieces:]
    rows = product_ref.shape[1]
    runs = max(len(got_refs), pieces)
    each = product_ref.shape[2] // runs
    for i in range(runs):
        at = slice(i * each, (i + 1) * each)
        got_ref, got_at = (got_refs[0], at) if len(got_refs) == 1 else (got_refs[i], slice(None))
        out_ref, out_at = (out_refs[0], at) if pieces == 1 else (out_refs[i], slice(None))
        out_ref[:rows, out_at] = (got_ref[:rows, got_at].astype(F32) + product_ref[0, :, at]).astype(BF16)
        if out_ref.shape[0] > rows:
            norm = jnp.sum(got_ref[rows:, got_at].astype(F32), axis=0, keepdims=True) + norm_ref[:1, at]
            put_norm(out_ref, rows, out_at, norm)


def added(got, product, norm, pieces):
    rows, columns = product.shape[1:]
    return pl.pallas_call(
        functools.partial(add_on, pieces=pieces),
        out_shape=[jax.ShapeDtypeStruct((got[0].shape[0], columns // pieces), BF16)] * pieces,
        in_specs=[VMEM] * (len(got) + 2),
        out_specs=[VMEM] * pieces,
        compiler_params=pltpu.CompilerParams(vmem_limit_bytes=8 << 20),
        cost_estimate=pl.CostEstimate(flops=rows * columns * 1000, bytes_accessed=2 << 20, transcendentals=0),
        name="add_on",
    )(*got, product, norm)


def finish(a_ref, b_ref, c_ref, d_ref, product_ref, norm_ref, out_ref, held_ref, sems):
    rows = product_ref.shape[1]
    step = rows // 2
    squares = norm_ref[:1, :]
    for ref in (a_ref, c_ref):
        squares = squares + jnp.sum(ref[rows:, :].astype(F32), axis=0, keepdims=True)
    norm = jnp.sqrt(squares)
    core = lax.axis_index("depth").astype(jnp.int32)
    stores = []
    for half, one, two in ((core, a_ref, d_ref), (1 - core, b_ref, c_ref)):
        for start in range(0, rows, step):
            at = pl.ds(start, step)
            total = product_ref[half, at] + one[at, :].astype(F32) + two[at, :].astype(F32)
            held_ref[len(stores)] = total / norm
            store = pltpu.make_async_copy(held_ref.at[len(stores)], out_ref.at[half, at], sems.at[len(stores)])
            store.start()
            stores.append(store)
    for store in stores:
        store.wait()


def finished(first, second, first_across, second_across, product, norm):
    _, rows, columns = product.shape
    return pl.pallas_call(
        finish,
        out_shape=jax.ShapeDtypeStruct(product.shape, F32),
        in_specs=[VMEM] * 6,
        out_specs=HBM,
        scratch_shapes=[pltpu.VMEM((4, rows // 2, columns), F32), pltpu.SemaphoreType.DMA((4,))],
        cost_estimate=pl.CostEstimate(flops=product.size * 100, bytes_accessed=4 << 20, transcendentals=0),
        compiler_params=pltpu.CompilerParams(vmem_limit_bytes=8 << 20),
        name="finish",
    )(first, second, first_across, second_across, product, norm)


def pack(spectrum_ref, wanted_ref, fraction_ref, out_ref, held_ref, wanted_held, fraction_held, sems):
    loads = []
    for i, (ref, held) in enumerate(((spectrum_ref, held_ref), (wanted_ref, wanted_held), (fraction_ref, fraction_held))):
        loads.append(pltpu.make_async_copy(ref, held, sems.at[i]))
    for load in loads:
        load.start()
    for load in loads:
        load.wait()
    rows = []
    for half in range(2):
        for start in range(0, held_ref.shape[1], LANES):
            rows.append(held_ref[half : half + 1, start : start + LANES])
    for ref in (wanted_held, fraction_held):
        for start in range(0, ref.shape[1], LANES):
            rows.append(ref[:, start : start + LANES].astype(F32))
    out_ref[...] = jnp.concatenate(rows, axis=0)


def packed(spectrum, wanted, fraction):
    arrays = (spectrum, wanted.reshape(1, -1), fraction.reshape(1, -1))
    rows = sum(x.size for x in arrays) // LANES
    return pl.pallas_call(
        pack,
        out_shape=pltpu.VMEM((rows, LANES), F32),
        in_specs=[HBM] * 3,
        out_specs=VMEM,
        scratch_shapes=[pltpu.VMEM(x.shape, x.dtype) for x in arrays] + [pltpu.SemaphoreType.DMA((3,))],
        compiler_params=pltpu.CompilerParams(vmem_limit_bytes=62 << 20),
        cost_estimate=pl.CostEstimate(flops=1000, bytes_accessed=400000, transcendentals=0),
        name="pack",
    )(*arrays)


def body(halves, spectrum, wanted, fraction):
    rows = halves.shape[1]
    ncols = lax.axis_size("col")
    ndepth = lax.axis_size("depth")
    nrows = lax.axis_size(ROW)
    columns = wanted.shape[0]
    reach = ncols // 2
    ring = ("col", "depth")

    def along(core, col, by):
        return (col + (by if core == 0 else -by)) % ncols

    straight = [(k * ndepth + c, along(c, k, 1) * ndepth + c) for k in range(ncols) for c in range(ndepth)]
    across = [(k * ndepth + c, along(c, k, 1) * ndepth + 1 - c) for k in range(ncols) for c in range(ndepth)]

    other = lax.ppermute(halves, "depth", [(0, 1), (1, 0)])
    pairs = []
    for r in range(nrows):
        for k in range(ncols):
            for c in range(ndepth):
                source = along(c, k, (r or nrows - 1) // 2) * ndepth + (c ^ ((r or nrows - 1) & 1))
                pairs.append((r * ncols * ndepth + source, r * ncols * ndepth + k * ndepth + c))
    mine = packed(spectrum, wanted, fraction)
    theirs = lax.ppermute(mine, ROW + ring, pairs)
    theirs = jnp.where(lax.axis_index(ROW) == 0, mine, theirs)
    last = lax.axis_index(ROW) == nrows - 1
    edge = [jnp.where(last, h[0, rows - 1], h[1, 0]).astype(F32).reshape(-1, LANES) for h in (halves, other)]
    parcel = jnp.concatenate([theirs] + edge, axis=0)
    blocks = lax.all_to_all(jnp.broadcast_to(parcel[None], (nrows,) + parcel.shape), ROW, 0, 0, tiled=True)

    multiplied = functools.partial(products, blocks=blocks, own=halves, other=other, columns=columns)
    (a,) = multiplied(("first",), step=reach, sends=True, tall=True)
    a = lax.ppermute(a, ring, straight)
    b, norm, *found = multiplied(("second",), step=reach - 1, sends=True)
    b = lax.ppermute(b, ring, straight)
    product, more = multiplied(("first",), step=reach - 1, found=found)
    (a,) = added([a], product, norm + more, 1)
    for step in range(reach - 2, 0, -1):
        a = lax.ppermute(a, ring, straight)
        product, norm, *found = multiplied(("second",), step=step)
        pieces = 1 if step > 1 else 2
        b, *b_across = added([b], product, norm, pieces)
        b = lax.ppermute(b, ring, straight)
        b_across = [lax.ppermute(x, ring, across) for x in b_across]
        product, more = multiplied(("first",), step=step, found=found)
        a, *a_across = added([a], product, norm + more, pieces)
    a = lax.ppermute(a, ring, straight)
    a_across = [lax.ppermute(x, ring, across) for x in a_across]
    product, norm = multiplied((0, 1), step=0, columns=columns // ndepth)
    return finished(a, b, a_across[0], b_across[0], product, norm)


def solution(mesh):
    split = Mesh(
        mesh.devices.reshape(4, 4, mesh.shape["col"], mesh.shape["depth"]), ("row_0", "row_1", "col", "depth")
    )
    in_specs = (P(None, ROW, ("col", "depth")), P(None, ("col", "depth")), P("col"), P("col"))
    out_specs = P(None, ROW, ("col", "depth"))
    return jax.shard_map(body, mesh=split, in_specs=in_specs, out_specs=out_specs, check_vma=False)
```
